256 devices in a mesh: expert: 64 (over y, z, core), gate: 4 (over x).
Axes of the slice: x: 4, y: 4, z: 8, core: 2. Of those that a mesh axis runs over, the one named last changes fastest.
Arguments:
- samples: bfloat16 [49152, 4096], P('expert', 'gate'), may hold values from -4 to 4
- gate_weight: bfloat16 [4096, 256], P('gate'), may hold values from -1 to 1
- expert_ids: int32 [49152, 2], P('expert'), may hold values from 0 to 255, all different within a row; in each aligned block of 768 rows (0 to 767, 768 to 1535, ...) at most 12 rows name the same one
- pad_mask: int32 [49152], P('expert'), may hold values 0 or 1
- up_weight: bfloat16 [256, 4096, 1024], P(('expert', 'gate')), may hold values from -0.09375 to 0.09375
- down_weight: bfloat16 [256, 1024, 1024], P(('expert', 'gate')), may hold values from -0.1875 to 0.1875
Outputs:
- combined: bfloat16 [49152, 1024], P('expert', 'gate')
The draws below stay inside these ranges and needn't reach their ends.
Inputs may be any that keep to these rules, and one draw needn't show every extreme that they name: `expert_ids`: each sample names two different experts; among the 768 samples of one index of expert no expert is named more than 12 times, a bound that some block reaches.
All inputs are finite; a program needn't handle non-finite values. No bound on the sum of `pad_mask` on one device may be relied on, other than what follows from the above.
Results may differ from the reference program's by a relative error of at most 0.0057.
Values may be sent and summed in bfloat16 or wider, within the bound.
A program may use at most 128 MiB of HBM per device.

```python
import math
import jax
import jax.numpy as jnp
import numpy as np
from jax import lax

D = 4096
H = 1024
OUT = 1024
ROWS_DEV = 768
EXPERTS = 256
CAP = 12
BATCH = 49152
N_EXPERT = 64


def draw_samples(key, part):
    inner = jax.random.fold_in(key, 3)
    drawn = jnp.clip(jax.random.normal(inner, (BATCH, D), jnp.float32), -4.0, 4.0)
    return drawn.astype(jnp.bfloat16)


def draw_gate_weight(key, part):
    inner = jax.random.fold_in(key, 5)
    spread_key = jax.random.fold_in(key, 6)
    scales = jnp.exp(jax.random.uniform(spread_key, (1, EXPERTS), jnp.float32, jnp.log(0.15), jnp.log(1.5)))
    drawn = jnp.clip(jax.random.normal(inner, (D, EXPERTS), jnp.float32), -4.0, 4.0)
    drawn = drawn * scales / jnp.sqrt(jnp.float32(D))
    return drawn.astype(jnp.bfloat16)


def place_ends(entries, rng, low, high):
    place = [jax.random.randint(jax.random.fold_in(rng, axis), (), 0, length) for axis, length in enumerate(entries.shape)]
    longest = entries.shape.index(max(entries.shape))
    neighbour = place[:longest] + [(place[longest] + 1) % entries.shape[longest]] + place[longest + 1:]
    return entries.at[tuple(place)].set(low).at[tuple(neighbour)].set(high)


def levels(key, extent, cuts, low, largest):
    def one(dim, blocks):
        draws = jax.random.uniform(jax.random.fold_in(jax.random.fold_in(key, 6), dim), (blocks,), jnp.float32, low / len(cuts), largest / len(cuts))
        return jnp.repeat(jnp.exp(draws), extent[dim] // blocks).reshape((-1,) + (1,) * (len(extent) - dim - 1))

    loudness = one(*cuts[0])
    for cut in cuts[1:]:
        loudness = loudness * one(*cut)
    return loudness


def routed_block(rng, own, number, rows, number_of, top, reach, skew):
    order = jax.random.permutation(rng, number_of)
    packed, usual = portions_of(number_of, rows * top, reach, skew, True), portions_of(number_of, rows * top, reach, skew, False)
    places = jnp.arange(number_of)

    def named(sizes, offset_by):
        used = int((sizes > 0).sum())
        fixed = max(1, used // 4)
        moved = fixed + (places - fixed + offset_by * (used - fixed)) % max(1, number_of - fixed)
        return jnp.zeros((number_of,), jnp.int32).at[order[jnp.where(places < fixed, places, moved)]].set(jnp.asarray(sizes, jnp.int32))

    sizes = jnp.where(number % 4 == 0, named(packed, number // 4), named(usual, number - number // 4 - 1))
    mixed = jax.random.permutation(jax.random.fold_in(own, 3), number_of)
    source_of, taker = mixed[0:number_of // 2 * 2:2], mixed[1:number_of // 2 * 2:2]
    room = jnp.minimum(sizes[source_of] - 1, reach - sizes[taker]) // 2
    room = jnp.where((source_of == order[0]) | (taker == order[0]) | (sizes[taker] == 0), 0, jnp.maximum(room, 0))
    moved = jax.random.randint(jax.random.fold_in(own, 4), (number_of // 2,), 0, 1 << 20) % (room + 1)
    sizes = sizes.at[source_of].add(-moved).at[taker].add(moved)
    labels = jnp.searchsorted(jnp.cumsum(sizes), jnp.arange(rows * top), side="right").astype(jnp.int32)
    listing = labels.reshape(top, rows).T
    listing = listing[jax.random.permutation(jax.random.fold_in(own, 1), rows)]
    offset_by = jax.random.randint(jax.random.fold_in(own, 2), (rows, 1), 0, top)
    return jnp.take_along_axis(listing, (jnp.arange(top)[None, :] + offset_by) % top, axis=1)


def portions_of(number_of, total, limit, slope, full):
    weights = [(1 << 20) // math.isqrt(standing ** slope) + 1 for standing in range(1, number_of + 1)]
    largest = limit if full else min(limit, max(-(-total // number_of), total * weights[0] // sum(weights)))
    least = 1 if total - largest >= number_of - 1 else 0
    counts, rest = [largest] + [least] * (number_of - 1), total - largest - least * (number_of - 1)
    while rest > 0:
        movable = [i for i in range(1, number_of) if counts[i] < largest] or [i for i in range(1, number_of) if counts[i] < limit]
        whole, budget = sum([weights[i] for i in movable]), rest
        for i in movable:
            addition = min(limit - counts[i], max(1, budget * weights[i] // whole), rest)
            counts[i] = counts[i] + addition
            rest = rest - addition
    return np.array(counts)


def noise(stream_key, extent, spread, most, cuts=(), kind=jnp.bfloat16):
    gain = levels(stream_key, extent, cuts, -0.22, 0.18) if cuts else 1.0
    drawn = jax.random.normal(stream_key, extent, jnp.float32) * spread * gain
    return jnp.minimum(jnp.maximum(drawn, -most), most).astype(kind)


def setup_inputs(seed: int = 0) -> dict:
    key_of = jax.random.split(jax.random.key(seed), 7)
    samples = draw_samples(jax.random.fold_in(key_of[6], 71), 0)
    gate_weight = draw_gate_weight(jax.random.fold_in(key_of[6], 71), 0)
    expert_ids_keys = jax.random.split(jax.random.fold_in(key_of[2], 1), BATCH // ROWS_DEV)
    expert_ids_turns = jax.random.permutation(jax.random.fold_in(key_of[2], 3), BATCH // ROWS_DEV)
    expert_ids = jax.vmap(lambda own, number: routed_block(jax.random.fold_in(key_of[2], 2), own, number, ROWS_DEV, EXPERTS, 2, CAP, 1))(expert_ids_keys, expert_ids_turns).reshape((BATCH, 2))
    pad_mask = place_ends((jax.random.randint(key_of[3], (BATCH,), 0, 8) < 7).astype(jnp.int32), jax.random.fold_in(key_of[3], 1), 0, 1)
    up_weight = noise(key_of[4], (EXPERTS, D, H), D ** -0.5, 0.09375, ((0, 256),))
    down_weight = noise(key_of[5], (EXPERTS, H, OUT), H ** -0.5, 0.1875, ((0, 256),))
    return {"samples": samples, "gate_weight": gate_weight, "expert_ids": expert_ids, "pad_mask": pad_mask, "up_weight": up_weight, "down_weight": down_weight}


def reference(samples, gate_weight, expert_ids, pad_mask, up_weight, down_weight):
    logits = jnp.dot(samples, gate_weight, preferred_element_type=jnp.float32)
    row_top = jnp.max(logits, axis=1, keepdims=True)
    row_total = jnp.sum(jnp.exp(logits - row_top), axis=1, keepdims=True)
    chosen = jnp.take_along_axis(logits, expert_ids, axis=1)
    factor = EXPERTS * jnp.exp(chosen - row_top) / row_total * pad_mask.astype(jnp.float32)[:, None]
    grouped = expert_ids.reshape(N_EXPERT, ROWS_DEV * 2)
    onehot = (grouped[:, :, None] == jnp.arange(EXPERTS, dtype=jnp.int32)[None, None, :]).astype(jnp.int32)
    slot_rank = jnp.sum(onehot * (jnp.cumsum(onehot, axis=1) - 1), axis=2)
    source_index = jnp.arange(N_EXPERT, dtype=jnp.int32)[:, None]
    position = (grouped * (N_EXPERT * CAP) + source_index * CAP + slot_rank).reshape(-1).astype(jnp.int32)
    row_index = jnp.repeat(jnp.arange(BATCH, dtype=jnp.int32), 2)
    owners = jnp.full((EXPERTS * N_EXPERT * CAP,), BATCH, jnp.int32).at[position].set(row_index)
    padded = jnp.concatenate([samples, jnp.zeros((1, D), samples.dtype)], axis=0)

    def expert_pass(operands):
        owner_block, first, second = operands
        slot_block = padded[owner_block]
        hidden = jnp.dot(slot_block, first, preferred_element_type=jnp.float32)
        active = jnp.maximum(hidden, 0.0).astype(jnp.bfloat16)
        return jnp.dot(active, second, preferred_element_type=jnp.float32).astype(jnp.bfloat16)

    results = lax.map(expert_pass, (owners.reshape(EXPERTS, N_EXPERT * CAP), up_weight, down_weight))
    flat_out = results.reshape(EXPERTS * N_EXPERT * CAP, OUT)
    picked = flat_out[position].astype(jnp.float32).reshape(BATCH, 2, OUT)
    return jnp.sum(factor[:, :, None] * picked, axis=1).astype(jnp.bfloat16)
```

```python
import functools

import jax
import jax.numpy as jnp
from jax import lax
from jax.experimental import pallas as pl
from jax.experimental.pallas import tpu as pltpu
from jax.sharding import PartitionSpec as P

MESH = pl.DeviceIdType.MESH
Y, Z, C, X = 4, 8, 2, 4
CAP = 12
F32, BF16, I32 = jnp.float32, jnp.bfloat16, jnp.int32
EXACT = dict(preferred_element_type=F32)


def iota(shape, dim):
    return lax.broadcasted_iota(I32, shape, dim)


def div(v, n):
    return lax.shift_right_logical(v * (-(-(1 << 17) // n)), 17)


def as_mask(cond):
    return jnp.where(cond, 1.0, 0.0).astype(BF16)


def kernel(
    samples, gate, ids, mask, up, down, out,
    sv, gv, w1, w2, near, hop, far, last,
    sb0, sb1, sb2, sb3, sb4, xb0, xb1, xb2, xb3, xb4,
    ob0, ob1, ob2, ob3, ob4, rb0, rb1, rb2, rb3, rb4,
    zs, zr, posb, rowb, pick, pickr, cols, lpart, lrecv, fac, act, acc,
    wsem, ssem, hsend, hrecv, isend, irecv, rsend, rrecv, zsend, zrecv, msend, mrecv,
):
    sb, xb = (sb0, sb1, sb2, sb3, sb4), (xb0, xb1, xb2, xb3, xb4)
    ob, rb = (ob0, ob1, ob2, ob3, ob4), (rb0, rb1, rb2, rb3, rb4)
    width = (16, 24, 24, 24, 16)
    ne = lax.axis_index("expert")
    x = lax.axis_index("gate")
    y, z, c = ne // (Z * C), (ne // C) % Z, ne % C
    half = Y * C * X * CAP // 2
    nf = sv.shape[0]
    rows = sv.shape[1]
    wide = sv.shape[2]
    share = rows // X

    def at_z(d):
        return (y * Z + (z + d) % Z) * C + c, x

    def in_plane(k):
        dy, dc, dx = k // (C * X), (k // X) % C, k % X
        y2, c2, x2 = (y + dy) % Y, (c + dc) % C, (x + dx) % X
        return y2, c2, x2, ((y2 * Z + z) * C + c2, x2)

    peers = Y * C * X
    mine = (y * C + c) * X + x
    source = x * (Y * C) + y * C + c

    def remote(src, dst, ss, rs, dev):
        return pltpu.make_async_remote_copy(
            src_ref=src, dst_ref=dst, send_sem=ss, recv_sem=rs, device_id=dev, device_id_type=MESH
        )

    def local(src, dst, sem):
        return pltpu.make_async_copy(src, dst, sem)

    fetch_s = [local(samples.at[:, pl.ds(f * wide, wide)], sv.at[f], ssem.at[f]) for f in range(nf)]
    for copy in fetch_s:
        copy.start()
    fetch_g = local(gate, gv, wsem.at[0])
    fetch_g.start()
    nt = w1.shape[0]
    fetch_1 = [
        local(up.at[0, :, pl.ds(j * w1.shape[2], w1.shape[2])], w1.at[j], wsem.at[1 + j]) for j in range(nt)
    ]
    fetch_2 = [
        local(down.at[0, :, pl.ds(j * w2.shape[2], w2.shape[2])], w2.at[j], wsem.at[1 + nt + j]) for j in range(nt)
    ]
    for copy in fetch_1 + fetch_2:
        copy.start()

    barrier = pltpu.get_barrier_semaphore()

    def greet(k, carry):
        pl.semaphore_signal(barrier, inc=1, device_id=in_plane(k)[3], device_id_type=MESH)
        return carry

    lax.fori_loop(1, peers, greet, 0)
    for d in range(1, Z):
        pl.semaphore_signal(barrier, inc=1, device_id=at_z(d), device_id_type=MESH)
    pl.semaphore_wait(barrier, peers - 1 + Z - 1)

    sign = (1, -1)

    def hop_copy(step, way, f):
        dev = at_z(sign[way])
        sems = hsend.at[way, step, f], hrecv.at[way, step, f]
        if step == 0:
            src, dst = sv.at[f], near.at[way, 0, f]
        elif step == 1:
            src, dst = near.at[way, 0, f], near.at[way, 1, f]
        elif step == 2:
            src, dst = hop.at[way, f], far.at[way, f]
        else:
            src, dst = far.at[way, f, pl.ds(0, half)], last.at[way, f]
        return remote(src, dst, *sems, dev)

    for f in range(nf):
        fetch_s[f].wait()
        if f == 0:
            hop_copy(0, 0, 0).start()
            hop_copy(0, 1, 0).start()

    experts = gate.shape[1]
    earlier = as_mask(iota((rows, rows), 0) < iota((rows, rows), 1))
    named = [as_mask(iota((experts, rows), 0) == ids[k : k + 1, :]) for k in range(2)]
    count = jnp.dot((named[0].astype(F32) + named[1].astype(F32)).astype(BF16), earlier, **EXACT)
    rowb[...] = jnp.zeros_like(rowb)
    for k in range(2):
        rank = jnp.sum(named[k].astype(F32) * count, axis=0, keepdims=True)
        posb[0, k : k + 1, :] = ids[k : k + 1, :] * CAP + rank.astype(I32)
        rowb[k : k + 1, :] = ids[k : k + 1, :].astype(F32)
        rowb[2 + k : 3 + k, :] = rank
    rowb[4:5, :] = mask[...].astype(F32)

    def pos_copy(d):
        return remote(posb.at[0], posb.at[d], msend.at[0], mrecv.at[0], at_z(d))

    for d in range(1, Z):
        pos_copy(d).start()
    for f in range(1, nf):
        hop_copy(0, 0, f).start()
        hop_copy(0, 1, f).start()

    same = as_mask(iota((rows, rows), 0) == iota((rows, rows), 1))
    turned = lax.dot_general(same, rowb[...].astype(BF16), (((1,), (1,)), ((), ())), **EXACT)
    cols[...] = turned.reshape(cols.shape)

    def target(shape, dim, n, a, plane):
        i = iota(shape, dim)
        if n == CAP:
            block, j = div(i, CAP * C * X), i
            return block * (Z * C * X * CAP - C * X * CAP) + plane * (C * X * CAP) + j
        d = div(i, n)
        s = i - d * n - a * CAP
        block = lax.shift_right_logical(d, 3)
        slot = block * (Z * C * X * CAP) + plane * (C * X * CAP) + (d - block * (C * X)) * CAP + s
        return jnp.where((s >= 0) & (s < CAP), slot, -1)

    def chooser(slots, d):
        p0, p1 = posb[d, 0:1, :], posb[d, 1:2, :]
        return as_mask((slots == p0) | (slots == p1))

    def send_in_plane(g):
        def one(k, carry):
            y2, c2, x2, dev = in_plane(k)
            remote(sb[g].at[(y2 * C + c2) * X + x2], xb[g].at[source], isend.at[g], irecv.at[g], dev).start()
            return carry

        lax.fori_loop(1, peers, one, 0)
        xb[g][source] = sb[g][mine]

    def put(g, f, value):
        n = width[g]
        sb[g][:, :, f * wide : (f + 1) * wide] = value.reshape(peers, n, wide).astype(BF16)

    pick[0, : peers * 16, :] = chooser(target((peers * 16, 1), 0, 16, 0, z), 0)
    for f in range(nf):
        put(0, f, jnp.dot(pick[0, : peers * 16, :], sv[f], **EXACT))
    send_in_plane(0)

    fetch_g.wait()
    logits = jnp.zeros((rows, experts), F32)
    for f in range(nf):
        logits = logits + jnp.dot(sv[f], gv[f * wide : (f + 1) * wide, :], **EXACT)
    lpart[...] = logits.reshape(lpart.shape)

    def along_x(d):
        return ne, (x + d) % X

    def logit_copy(d):
        return remote(lpart.at[(x + d) % X], lrecv.at[d - 1], msend.at[1], mrecv.at[1], along_x(d))

    for d in range(1, X):
        logit_copy(d).start()

    def relay(step, f):
        for way in range(2):
            hop_copy(step, way, f).wait_recv()
            if step < 3:
                hop_copy(step + 1, way, f).start()

    m_of = [Y * C * n for n in width]

    def expert(g):
        n, m = width[g], m_of[g]
        remote(sb[g].at[pl.ds(0, peers - 1)], xb[g].at[pl.ds(0, peers - 1)], isend.at[g], irecv.at[g], along_x(1)).wait_recv()

        def first(j, carry):
            total = jnp.zeros((m, w1.shape[2]), F32)
            for xs in range(X):
                part = xb[g][xs * Y * C : (xs + 1) * Y * C].reshape(m, nf * wide)
                total = total + jnp.dot(part, w1[j, xs * nf * wide : (xs + 1) * nf * wide, :], **EXACT)
            act[j, 0:m, :] = jnp.maximum(total, 0.0).astype(BF16)
            return carry

        lax.fori_loop(0, nt, first, 0)

        def second(j, carry):
            total = jnp.zeros((m, w2.shape[2]), F32)
            for i in range(nt):
                total = total + jnp.dot(act[i, 0:m, :], w2[j, i * w1.shape[2] : (i + 1) * w1.shape[2], :], **EXACT)
            ob[g][j] = total.reshape(Y * C, n, w2.shape[2]).astype(BF16)
            return carry

        lax.fori_loop(0, nt, second, 0)

        def one(k, carry):
            y2, c2, x2, dev = in_plane(k)
            remote(ob[g].at[x2, y2 * C + c2], rb[g].at[mine], rsend.at[g], rrecv.at[g], dev).start()
            return carry

        lax.fori_loop(1, peers, one, 0)
        rb[g][mine] = ob[g][x, y * C + c]

    def back_in_plane(g):
        block = rb[g].at[pl.ds(0, peers - 1)]
        remote(block, block, rsend.at[g], rrecv.at[g], along_x(1)).wait_recv()

    def back_copy(d):
        return remote(zs.at[d], zr.at[d], zsend.at[d], zrecv.at[d], at_z(-d))

    def send_back(g, sources):
        n = width[g]
        q, i = iota((2 * half, peers * n), 0), iota((2 * half, peers * n), 1)
        base = q + div(q, CAP) * (n - CAP)
        got = rb[g][...].reshape(peers * n, rb[g].shape[2])
        for a, d in enumerate(sources):
            zs[d] = jnp.dot(as_mask(i == base + a * CAP), got, **EXACT).astype(BF16)
            back_copy(d).start()

    def add_up(plane, n, values, fresh=False):
        slots = target((1, values.shape[0]), 1, n, 0, plane)
        for k in range(2):
            col = cols[...].reshape(rows, 8)
            p = (col[:, k : k + 1] * CAP + col[:, 2 + k : 3 + k]).astype(I32)
            term = jnp.dot(as_mask(p == slots), values, **EXACT)
            if fresh:
                acc[k] = term
            else:
                acc[k] += term

    relay(0, 0)
    relay(0, 1)
    for copy in fetch_1 + fetch_2:
        copy.wait()
    expert(0)
    relay(0, 2)
    relay(0, 3)
    remote(posb.at[pl.ds(0, Z - 1)], posb.at[pl.ds(0, Z - 1)], msend.at[0], mrecv.at[0], along_x(1)).wait_recv()

    def choose_pair(g, dist):
        n = width[g]
        for a, d in enumerate((dist, Z - dist)):
            pick[a] = chooser(target((peers * n, 1), 0, n, a, z), d)
        for f in range(nf):
            put(
                g, f,
                jnp.dot(pick[0], near[0, dist - 1, f], **EXACT) + jnp.dot(pick[1], near[1, dist - 1, f], **EXACT),
            )
        send_in_plane(g)

    choose_pair(1, 1)

    for way in range(2):
        d = 2 if way == 0 else Z - 2
        p3, p4 = (z + sign[way]) % Z, (z + 2 * sign[way]) % Z
        q4 = target((2 * half, 1), 0, CAP, 0, p4)
        pickr[way, 0:half, :] = chooser(q4[way * half : (way + 1) * half], d)
        pickr[way, half:, :] = chooser(target((2 * half, 1), 0, CAP, 0, p3), d)

    remote(lrecv, lrecv, msend.at[1], mrecv.at[1], along_x(1)).wait_recv()
    logit = lpart[x] + lrecv[0] + lrecv[1] + lrecv[2]
    row_top = jnp.max(logit, axis=1, keepdims=True)
    term = jnp.exp(logit - row_top)
    row_total = jnp.sum(term, axis=1, keepdims=True)
    col = cols[x]
    lane = iota((share, experts), 1)
    both = []
    for k in range(2):
        chosen = jnp.sum(jnp.where(lane == col[:, k : k + 1].astype(I32), term, 0.0), axis=1, keepdims=True)
        both.append(experts * chosen / row_total * col[:, 4:5])
    wide_lane = iota((share, fac.shape[2]), 1)
    fac[x] = jnp.where(wide_lane == 0, both[0], jnp.where(wide_lane == 1, both[1], 0.0))

    def factor_copy(d):
        return remote(fac.at[x], fac.at[x], msend.at[2], mrecv.at[2], along_x(d))

    for d in range(1, X):
        factor_copy(d).start()

    back_in_plane(0)
    add_up(z, 16, rb[0][...].reshape(peers * 16, rb[0].shape[2]), True)

    def relay_chosen(f):
        for way in range(2):
            hop_copy(1, way, f).wait_recv()
            hop[way, f] = jnp.dot(pickr[way], near[way, 1, f], **EXACT).astype(BF16)
            hop_copy(2, way, f).start()

    relay_chosen(0)
    relay_chosen(1)
    expert(1)
    relay_chosen(2)
    relay_chosen(3)
    back_in_plane(1)
    send_back(1, (1, Z - 1))
    choose_pair(2, 2)
    relay(2, 0)
    relay(2, 1)
    expert(2)
    relay(2, 2)
    relay(2, 3)

    def spread(n, a, count):
        i, q = iota((count // CAP * n, count), 0), iota((count // CAP * n, count), 1)
        return as_mask(i == q + div(q, CAP) * (n - CAP) + a * CAP)

    for a in range(2):
        pick[a, :, 0 : 2 * half] = spread(24, a, 2 * half)
    for f in range(nf):
        put(
            3, f,
            jnp.dot(pick[0, :, 0 : 2 * half], far[0, f, half:], **EXACT)
            + jnp.dot(pick[1, :, 0 : 2 * half], far[1, f, half:], **EXACT),
        )
    send_in_plane(3)
    back_in_plane(2)
    send_back(2, (2, Z - 2))

    relay(3, 0)
    relay(3, 1)
    relay(3, 2)
    relay(3, 3)
    grow = spread(16, 0, half)
    for f in range(nf):
        for way in range(2):
            half_peers = peers // 2
            sb[4][way * half_peers : (way + 1) * half_peers, :, f * wide : (f + 1) * wide] = (
                jnp.dot(grow, last[way, f], **EXACT).reshape(half_peers, 16, wide).astype(BF16)
            )
    send_in_plane(4)
    expert(3)
    back_in_plane(3)
    send_back(3, (3, Z - 3))
    expert(4)
    back_in_plane(4)
    send_back(4, (4,))

    for d in (1, 7, 2, 6, 3, 5, 4):
        back_copy(d).wait_recv()
        add_up((z + d) % Z, CAP, zr[d])

    block = fac.at[pl.ds(0, X - 1)]
    remote(block, block, msend.at[2], mrecv.at[2], along_x(1)).wait_recv()
    scale = fac[...].reshape(rows, fac.shape[2])
    out[...] = (scale[:, 0:1] * acc[0] + scale[:, 1:2] * acc[1]).astype(out.dtype)

    for step in range(4):
        for way in range(2):
            for f in range(nf):
                hop_copy(step, way, f).wait_send()
    remote(posb.at[pl.ds(0, Z - 1)], posb.at[pl.ds(0, Z - 1)], msend.at[0], mrecv.at[0], along_x(1)).wait_send()
    remote(lrecv, lrecv, msend.at[1], mrecv.at[1], along_x(1)).wait_send()
    remote(block, block, msend.at[2], mrecv.at[2], along_x(1)).wait_send()
    for g in range(5):
        sent = sb[g].at[pl.ds(0, peers - 1)]
        remote(sent, sent, isend.at[g], irecv.at[g], along_x(1)).wait_send()
        sent = rb[g].at[pl.ds(0, peers - 1)]
        remote(sent, sent, rsend.at[g], rrecv.at[g], along_x(1)).wait_send()
    for d in range(1, Z):
        back_copy(d).wait_send()


def per_device(samples, gate_weight, expert_ids, pad_mask, up_weight, down_weight):
    rows, share = samples.shape
    experts = gate_weight.shape[1]
    depth, hidden = up_weight.shape[1:]
    columns = down_weight.shape[2] // X
    peers = Y * C * X
    nf = 4
    wide = share // nf
    width = (16, 24, 24, 24, 16)
    slots = peers * CAP
    dma = pltpu.SemaphoreType.DMA
    any_space = pl.BlockSpec(memory_space=pl.ANY)
    vmem = pl.BlockSpec(memory_space=pltpu.VMEM)
    scratch = [
        pltpu.VMEM((nf, rows, wide), BF16),
        pltpu.VMEM(gate_weight.shape, BF16),
        pltpu.VMEM((4, depth, hidden // 4), BF16),
        pltpu.VMEM((4, hidden, columns), BF16),
        pltpu.VMEM((2, 2, nf, rows, wide), BF16),
        pltpu.VMEM((2, nf, slots * 3 // 2, wide), BF16),
        pltpu.VMEM((2, nf, slots * 3 // 2, wide), BF16),
        pltpu.VMEM((2, nf, slots // 2, wide), BF16),
    ]
    scratch += [pltpu.VMEM((peers, n, share), BF16) for n in width]
    scratch += [pltpu.VMEM((peers, n, share), BF16) for n in width]
    scratch += [pltpu.VMEM((X, Y * C, n, columns), BF16) for n in width]
    scratch += [pltpu.VMEM((peers, n, columns), BF16) for n in width]
    scratch += [
        pltpu.VMEM((Z, slots, columns), BF16),
        pltpu.VMEM((Z, slots, columns), BF16),
        pltpu.VMEM((Z, 2, rows), I32),
        pltpu.VMEM((8, rows), F32),
        pltpu.VMEM((2, peers * 24, rows), BF16),
        pltpu.VMEM((2, slots * 3 // 2, rows), BF16),
        pltpu.VMEM((X, rows // X, 8), F32),
        pltpu.VMEM((X, rows // X, experts), F32),
        pltpu.VMEM((X - 1, rows // X, experts), F32),
        pltpu.VMEM((X, rows // X, 128), F32),
        pltpu.VMEM((4, Y * C * 24, hidden // 4), BF16),
        pltpu.VMEM((2, rows, columns), F32),
    ]
    scratch += [
        dma((9,)), dma((nf,)), dma((2, 4, nf)), dma((2, 4, nf)), dma((5,)), dma((5,)),
        dma((5,)), dma((5,)), dma((Z,)), dma((Z,)), dma((3,)), dma((3,)),
    ]
    return pl.pallas_call(
        kernel,
        out_shape=jax.ShapeDtypeStruct((rows, columns), BF16),
        in_specs=[any_space, any_space, vmem, vmem, any_space, any_space],
        out_specs=vmem,
        scratch_shapes=scratch,
        compiler_params=pltpu.CompilerParams(
            collective_id=0, has_side_effects=True, vmem_limit_bytes=67043328
        ),
    )(samples, gate_weight, expert_ids.T, pad_mask.reshape(1, rows), up_weight, down_weight)


def solution(mesh):
    placed = (
        P("expert", "gate"),
        P("gate", None),
        P("expert", None),
        P("expert"),
        P(("expert", "gate"), None, None),
        P(("expert", "gate"), None, None),
    )
    return jax.shard_map(
        per_device, mesh=mesh, in_specs=placed, out_specs=P("expert", "gate"), check_vma=False
    )
```

```python
import jax
import jax.numpy as jnp
from jax import lax
from jax.experimental import pallas as pl
from jax.experimental.pallas import tpu as pltpu
from jax.sharding import PartitionSpec as P

MESH = pl.DeviceIdType.MESH
Y, Z, C, X = 4, 8, 2, 4
CAP = 12
F32, BF16, I32 = jnp.float32, jnp.bfloat16, jnp.int32
EXACT = dict(preferred_element_type=F32)


def iota(shape, dim):
    return lax.broadcasted_iota(I32, shape, dim)


def div(v, n):
    return lax.shift_right_logical(v * (-(-(1 << 17) // n)), 17)


def as_mask(cond):
    return jnp.where(cond, 1.0, 0.0).astype(BF16)


def kernel(
    samples, gate, ids, mask, up, down, out,
    sv, gv, w1, w2, near, hop, far, last,
    sb0, sb1, sb2, sb3, sb4, xb0, xb1, xb2, xb3, xb4,
    ob0, ob1, ob2, ob3, ob4, rb0, rb1, rb2, rb3, rb4,
    zs, zr, posb, rowb, pick, pickr, cols, lpart, lrecv, fac, act, acc,
    wsem, ssem, hsend, hrecv, isend, irecv, rsend, rrecv, zsend, zrecv, msend, mrecv,
):
    sb, xb = (sb0, sb1, sb2, sb3, sb4), (xb0, xb1, xb2, xb3, xb4)
    ob, rb = (ob0, ob1, ob2, ob3, ob4), (rb0, rb1, rb2, rb3, rb4)
    width = (16, 24, 24, 24, 16)
    ne = lax.axis_index("expert")
    x = lax.axis_index("gate")
    y, z, c = ne // (Z * C), (ne // C) % Z, ne % C
    half = Y * C * X * CAP // 2
    nf = sv.shape[0]
    rows = sv.shape[1]
    wide = sv.shape[2]
    share = rows // X

    def at_z(d):
        return (y * Z + (z + d) % Z) * C + c, x

    def in_plane(k):
        dy, dc, dx = k // (C * X), (k // X) % C, k % X
        y2, c2, x2 = (y + dy) % Y, (c + dc) % C, (x + dx) % X
        return y2, c2, x2, ((y2 * Z + z) * C + c2, x2)

    peers = Y * C * X
    mine = (y * C + c) * X + x
    source = x * (Y * C) + y * C + c

    def remote(src, dst, ss, rs, dev):
        return pltpu.make_async_remote_copy(
            src_ref=src, dst_ref=dst, send_sem=ss, recv_sem=rs, device_id=dev, device_id_type=MESH
        )

    def local(src, dst, sem):
        return pltpu.make_async_copy(src, dst, sem)

    fetch_s = [local(samples.at[:, pl.ds(f * wide, wide)], sv.at[f], ssem.at[f]) for f in range(nf)]
    for copy in fetch_s:
        copy.start()
    fetch_g = local(gate, gv, wsem.at[0])
    fetch_g.start()
    nt = w1.shape[0]
    fetch_1 = [
        local(up.at[0, :, pl.ds(j * w1.shape[2], w1.shape[2])], w1.at[j], wsem.at[1 + j]) for j in range(nt)
    ]
    fetch_2 = [
        local(down.at[0, :, pl.ds(j * w2.shape[2], w2.shape[2])], w2.at[j], wsem.at[1 + nt + j]) for j in range(nt)
    ]
    for copy in fetch_1 + fetch_2:
        copy.start()

    barrier = pltpu.get_barrier_semaphore()

    def greet(k, carry):
        pl.semaphore_signal(barrier, inc=1, device_id=in_plane(k)[3], device_id_type=MESH)
        return carry

    lax.fori_loop(1, peers, greet, 0)
    for d in range(1, Z):
        pl.semaphore_signal(barrier, inc=1, device_id=at_z(d), device_id_type=MESH)
    with jax.named_scope("greet"):
        pl.semaphore_wait(barrier, peers - 1 + Z - 1)

    sign = (1, -1)

    def hop_copy(step, way, f):
        dev = at_z(sign[way])
        sems = hsend.at[way, step, f], hrecv.at[way, step, f]
        if step == 0:
            src, dst = sv.at[f], near.at[way, 0, f]
        elif step == 1:
            src, dst = near.at[way, 0, f], near.at[way, 1, f]
        elif step == 2:
            src, dst = hop.at[way, f], far.at[way, f]
        else:
            src, dst = far.at[way, f, pl.ds(0, half)], last.at[way, f]
        return remote(src, dst, *sems, dev)

    for f in range(nf):
        fetch_s[f].wait()
        if f == 0:
            hop_copy(0, 0, 0).start()
            hop_copy(0, 1, 0).start()

    experts = gate.shape[1]
    earlier = as_mask(iota((rows, rows), 0) < iota((rows, rows), 1))
    named = [as_mask(iota((experts, rows), 0) == ids[k : k + 1, :]) for k in range(2)]
    count = jnp.dot((named[0].astype(F32) + named[1].astype(F32)).astype(BF16), earlier, **EXACT)
    rowb[...] = jnp.zeros_like(rowb)
    for k in range(2):
        rank = jnp.sum(named[k].astype(F32) * count, axis=0, keepdims=True)
        posb[0, k : k + 1, :] = ids[k : k + 1, :] * CAP + rank.astype(I32)
        rowb[k : k + 1, :] = ids[k : k + 1, :].astype(F32)
        rowb[2 + k : 3 + k, :] = rank
    rowb[4:5, :] = mask[...].astype(F32)

    def pos_copy(d):
        return remote(posb.at[0], posb.at[d], msend.at[0], mrecv.at[0], at_z(d))

    for d in range(1, Z):
        pos_copy(d).start()
    for f in range(1, nf):
        hop_copy(0, 0, f).start()
        hop_copy(0, 1, f).start()

    same = as_mask(iota((rows, rows), 0) == iota((rows, rows), 1))
    turned = lax.dot_general(same, rowb[...].astype(BF16), (((1,), (1,)), ((), ())), **EXACT)
    cols[...] = turned.reshape(cols.shape)

    def target(shape, dim, n, a, plane):
        i = iota(shape, dim)
        if n == CAP:
            block, j = div(i, CAP * C * X), i
            return block * (Z * C * X * CAP - C * X * CAP) + plane * (C * X * CAP) + j
        d = div(i, n)
        s = i - d * n - a * CAP
        block = lax.shift_right_logical(d, 3)
        slot = block * (Z * C * X * CAP) + plane * (C * X * CAP) + (d - block * (C * X)) * CAP + s
        return jnp.where((s >= 0) & (s < CAP), slot, -1)

    def chooser(slots, d):
        p0, p1 = posb[d, 0:1, :], posb[d, 1:2, :]
        return as_mask((slots == p0) | (slots == p1))

    def put(g, f, value):
        sb[g][f] = value.reshape(peers, width[g], wide).astype(BF16)

    def send_in_plane(g, f):
        def one(k, carry):
            y2, c2, x2, dev = in_plane(k)
            to = (y2 * C + c2) * X + x2
            remote(sb[g].at[f, to], xb[g].at[f, source], isend.at[g, f], irecv.at[g, f], dev).start()
            return carry

        lax.fori_loop(1, peers, one, 0)
        xb[g][f, source] = sb[g][f, mine]

    def dispatched(g, f):
        part = xb[g].at[f, pl.ds(0, peers - 1)]
        return remote(part, part, isend.at[g, f], irecv.at[g, f], along_x(1))

    def along_x(d):
        return ne, (x + d) % X

    pick[0, : peers * 16, :] = chooser(target((peers * 16, 1), 0, 16, 0, z), 0)
    for f in range(nf):
        put(0, f, jnp.dot(pick[0, : peers * 16, :], sv[f], **EXACT))
        send_in_plane(0, f)

    fetch_g.wait()
    logits = jnp.zeros((rows, experts), F32)
    for f in range(nf):
        logits = logits + jnp.dot(sv[f], gv[f * wide : (f + 1) * wide, :], **EXACT)
    lpart[...] = logits.reshape(lpart.shape)

    def logit_copy(d):
        return remote(lpart.at[(x + d) % X], lrecv.at[d - 1], msend.at[1], mrecv.at[1], along_x(d))

    for d in range(1, X):
        logit_copy(d).start()

    m_of = [Y * C * n for n in width]

    def expert(g):
        n, m = width[g], m_of[g]
        for f in range(nf):
            dispatched(g, f).wait_recv()

        def first(j, carry):
            total = jnp.zeros((m, w1.shape[2]), F32)
            for xs in range(X):
                group = slice(xs * Y * C, (xs + 1) * Y * C)
                part = jnp.concatenate([xb[g][f, group].reshape(m, wide) for f in range(nf)], axis=1)
                total = total + jnp.dot(part, w1[j, xs * nf * wide : (xs + 1) * nf * wide, :], **EXACT)
            act[j, 0:m, :] = jnp.maximum(total, 0.0).astype(BF16)
            return carry

        lax.fori_loop(0, nt, first, 0)

        def second(j, carry):
            total = jnp.zeros((m, w2.shape[2]), F32)
            for i in range(nt):
                total = total + jnp.dot(act[i, 0:m, :], w2[j, i * w1.shape[2] : (i + 1) * w1.shape[2], :], **EXACT)
            ob[g][j] = total.reshape(Y * C, n, w2.shape[2]).astype(BF16)
            return carry

        lax.fori_loop(0, nt, second, 0)

        def one(k, carry):
            y2, c2, x2, dev = in_plane(k)
            remote(ob[g].at[x2, y2 * C + c2], rb[g].at[mine], rsend.at[g], rrecv.at[g], dev).start()
            return carry

        lax.fori_loop(1, peers, one, 0)
        rb[g][mine] = ob[g][x, y * C + c]

    def back_in_plane(g):
        block = rb[g].at[pl.ds(0, peers - 1)]
        remote(block, block, rsend.at[g], rrecv.at[g], along_x(1)).wait_recv()

    def back_copy(d):
        return remote(zs.at[d], zr.at[d], zsend.at[d], zrecv.at[d], at_z(-d))

    def send_back(g, sources):
        n = width[g]
        q, i = iota((2 * half, peers * n), 0), iota((2 * half, peers * n), 1)
        base = q + div(q, CAP) * (n - CAP)
        got = rb[g][...].reshape(peers * n, rb[g].shape[2])
        for a, d in enumerate(sources):
            zs[d] = jnp.dot(as_mask(i == base + a * CAP), got, **EXACT).astype(BF16)
            back_copy(d).start()

    def add_up(plane, n, values, fresh=False):
        slots = target((1, values.shape[0]), 1, n, 0, plane)
        for k in range(2):
            col = cols[...].reshape(rows, 8)
            p = (col[:, k : k + 1] * CAP + col[:, 2 + k : 3 + k]).astype(I32)
            term = jnp.dot(as_mask(p == slots), values, **EXACT)
            if fresh:
                acc[k] = term
            else:
                acc[k] += term

    remote(posb.at[pl.ds(0, Z - 1)], posb.at[pl.ds(0, Z - 1)], msend.at[0], mrecv.at[0], along_x(1)).wait_recv()

    def choose_pair(g, dist):
        n = width[g]
        for a, d in enumerate((dist, Z - dist)):
            pick[a] = chooser(target((peers * n, 1), 0, n, a, z), d)

    def put_pair(g, dist, f):
        put(
            g, f,
            jnp.dot(pick[0], near[0, dist - 1, f], **EXACT) + jnp.dot(pick[1], near[1, dist - 1, f], **EXACT),
        )
        send_in_plane(g, f)

    def first_hop(f):
        for way in range(2):
            hop_copy(0, way, f).wait_recv()
            hop_copy(1, way, f).start()
        put_pair(1, 1, f)

    def second_hop(f):
        for way in range(2):
            hop_copy(1, way, f).wait_recv()
            hop[way, f] = jnp.dot(pickr[way], near[way, 1, f], **EXACT).astype(BF16)
            hop_copy(2, way, f).start()
        put_pair(2, 2, f)

    def spread(n, a, count):
        i, q = iota((count // CAP * n, count), 0), iota((count // CAP * n, count), 1)
        return as_mask(i == q + div(q, CAP) * (n - CAP) + a * CAP)

    def third_hop(f):
        for way in range(2):
            hop_copy(2, way, f).wait_recv()
            hop_copy(3, way, f).start()
        put(
            3, f,
            jnp.dot(pick[0, :, 0 : 2 * half], far[0, f, half:], **EXACT)
            + jnp.dot(pick[1, :, 0 : 2 * half], far[1, f, half:], **EXACT),
        )
        send_in_plane(3, f)

    def fourth_hop(f):
        half_peers = peers // 2
        grow = pick[0, 0 : half_peers * 16, 2 * half : 3 * half]
        for way in range(2):
            hop_copy(3, way, f).wait_recv()
            sb[4][f, way * half_peers : (way + 1) * half_peers] = (
                jnp.dot(grow, last[way, f], **EXACT).reshape(half_peers, 16, wide).astype(BF16)
            )
        send_in_plane(4, f)

    choose_pair(1, 1)
    first_hop(0)
    first_hop(1)
    for copy in fetch_1 + fetch_2:
        copy.wait()
    expert(0)
    first_hop(2)

    for way in range(2):
        d = 2 if way == 0 else Z - 2
        p3, p4 = (z + sign[way]) % Z, (z + 2 * sign[way]) % Z
        q4 = target((2 * half, 1), 0, CAP, 0, p4)
        pickr[way, 0:half, :] = chooser(q4[way * half : (way + 1) * half], d)
        pickr[way, half:, :] = chooser(target((2 * half, 1), 0, CAP, 0, p3), d)

    remote(lrecv, lrecv, msend.at[1], mrecv.at[1], along_x(1)).wait_recv()
    logit = lpart[x] + lrecv[0] + lrecv[1] + lrecv[2]
    row_top = jnp.max(logit, axis=1, keepdims=True)
    term = jnp.exp(logit - row_top)
    row_total = jnp.sum(term, axis=1, keepdims=True)
    col = cols[x]
    lane = iota((share, experts), 1)
    both = []
    for k in range(2):
        chosen = jnp.sum(jnp.where(lane == col[:, k : k + 1].astype(I32), term, 0.0), axis=1, keepdims=True)
        both.append(experts * chosen / row_total * col[:, 4:5])
    wide_lane = iota((share, fac.shape[2]), 1)
    fac[x] = jnp.where(wide_lane == 0, both[0], jnp.where(wide_lane == 1, both[1], 0.0))

    def factor_copy(d):
        return remote(fac.at[x], fac.at[x], msend.at[2], mrecv.at[2], along_x(d))

    for d in range(1, X):
        factor_copy(d).start()

    back_in_plane(0)
    add_up(z, 16, rb[0][...].reshape(peers * 16, rb[0].shape[2]), True)

    def gather_back(d):
        back_copy(d).wait_recv()
        add_up((z + d) % Z, CAP, zr[d])

    first_hop(3)
    choose_pair(2, 2)
    second_hop(0)
    expert(1)
    second_hop(1)
    back_in_plane(1)
    send_back(1, (1, Z - 1))
    second_hop(2)
    second_hop(3)
    for a in range(2):
        pick[a, :, 0 : 2 * half] = spread(24, a, 2 * half)
    pick[0, 0 : peers * 8, 2 * half : 3 * half] = spread(16, 0, half)
    third_hop(0)
    expert(2)
    third_hop(1)
    third_hop(2)
    back_in_plane(2)
    send_back(2, (2, Z - 2))
    third_hop(3)
    gather_back(1)
    gather_back(Z - 1)
    for f in range(nf):
        fourth_hop(f)
    expert(3)
    expert(4)
    back_in_plane(3)
    send_back(3, (3, Z - 3))
    back_in_plane(4)
    send_back(4, (4,))
    for d in (2, 6, 3, 5, 4):
        gather_back(d)

    block = fac.at[pl.ds(0, X - 1)]
    remote(block, block, msend.at[2], mrecv.at[2], along_x(1)).wait_recv()
    scale = fac[...].reshape(rows, fac.shape[2])
    out[...] = (scale[:, 0:1] * acc[0] + scale[:, 1:2] * acc[1]).astype(out.dtype)

    for step in range(4):
        for way in range(2):
            for f in range(nf):
                hop_copy(step, way, f).wait_send()
    remote(posb.at[pl.ds(0, Z - 1)], posb.at[pl.ds(0, Z - 1)], msend.at[0], mrecv.at[0], along_x(1)).wait_send()
    remote(lrecv, lrecv, msend.at[1], mrecv.at[1], along_x(1)).wait_send()
    remote(block, block, msend.at[2], mrecv.at[2], along_x(1)).wait_send()
    for g in range(5):
        for f in range(nf):
            dispatched(g, f).wait_send()
        sent = rb[g].at[pl.ds(0, peers - 1)]
        remote(sent, sent, rsend.at[g], rrecv.at[g], along_x(1)).wait_send()
    for d in range(1, Z):
        back_copy(d).wait_send()


def per_device(samples, gate_weight, expert_ids, pad_mask, up_weight, down_weight):
    rows, share = samples.shape
    experts = gate_weight.shape[1]
    depth, hidden = up_weight.shape[1:]
    columns = down_weight.shape[2] // X
    peers = Y * C * X
    nf = 4
    wide = share // nf
    width = (16, 24, 24, 24, 16)
    slots = peers * CAP
    dma = pltpu.SemaphoreType.DMA
    any_space = pl.BlockSpec(memory_space=pl.ANY)
    vmem = pl.BlockSpec(memory_space=pltpu.VMEM)
    scratch = [
        pltpu.VMEM((nf, rows, wide), BF16),
        pltpu.VMEM(gate_weight.shape, BF16),
        pltpu.VMEM((4, depth, hidden // 4), BF16),
        pltpu.VMEM((4, hidden, columns), BF16),
        pltpu.VMEM((2, 2, nf, rows, wide), BF16),
        pltpu.VMEM((2, nf, slots * 3 // 2, wide), BF16),
        pltpu.VMEM((2, nf, slots * 3 // 2, wide), BF16),
        pltpu.VMEM((2, nf, slots // 2, wide), BF16),
    ]
    scratch += [pltpu.VMEM((nf, peers, n, wide), BF16) for n in width]
    scratch += [pltpu.VMEM((nf, peers, n, wide), BF16) for n in width]
    scratch += [pltpu.VMEM((X, Y * C, n, columns), BF16) for n in width]
    scratch += [pltpu.VMEM((peers, n, columns), BF16) for n in width]
    scratch += [
        pltpu.VMEM((Z, slots, columns), BF16),
        pltpu.VMEM((Z, slots, columns), BF16),
        pltpu.VMEM((Z, 2, rows), I32),
        pltpu.VMEM((8, rows), F32),
        pltpu.VMEM((2, peers * 24, rows), BF16),
        pltpu.VMEM((2, slots * 3 // 2, rows), BF16),
        pltpu.VMEM((X, rows // X, 8), F32),
        pltpu.VMEM((X, rows // X, experts), F32),
        pltpu.VMEM((X - 1, rows // X, experts), F32),
        pltpu.VMEM((X, rows // X, 128), F32),
        pltpu.VMEM((4, Y * C * 24, hidden // 4), BF16),
        pltpu.VMEM((2, rows, columns), F32),
    ]
    scratch += [
        dma((9,)), dma((nf,)), dma((2, 4, nf)), dma((2, 4, nf)), dma((5, nf)), dma((5, nf)),
        dma((5,)), dma((5,)), dma((Z,)), dma((Z,)), dma((3,)), dma((3,)),
    ]
    return pl.pallas_call(
        kernel,
        out_shape=jax.ShapeDtypeStruct((rows, columns), BF16),
        in_specs=[any_space, any_space, vmem, vmem, any_space, any_space],
        out_specs=vmem,
        scratch_shapes=scratch,
        compiler_params=pltpu.CompilerParams(
            collective_id=0, has_side_effects=True, vmem_limit_bytes=67043328
        ),
    )(samples, gate_weight, expert_ids.T, pad_mask.reshape(1, rows), up_weight, down_weight)


def solution(mesh):
    placed = (
        P("expert", "gate"),
        P("gate", None),
        P("expert", None),
        P("expert"),
        P(("expert", "gate"), None, None),
        P(("expert", "gate"), None, None),
    )
    return jax.shard_map(
        per_device, mesh=mesh, in_specs=placed, out_specs=P("expert", "gate"), check_vma=False
    )
```

```python
import jax
import jax.numpy as jnp
from jax import lax
from jax.experimental import pallas as pl
from jax.experimental.pallas import tpu as pltpu
from jax.sharding import PartitionSpec as P

MESH = pl.DeviceIdType.MESH
Y, Z, C, X = 4, 8, 2, 4
CAP = 12
F32, BF16, I32 = jnp.float32, jnp.bfloat16, jnp.int32
EXACT = dict(preferred_element_type=F32)


def iota(shape, dim):
    return lax.broadcasted_iota(I32, shape, dim)


def div(v, n):
    return lax.shift_right_logical(v * (-(-(1 << 17) // n)), 17)


def as_mask(cond):
    return jnp.where(cond, 1.0, 0.0).astype(BF16)


def kernel(
    samples, gate, ids, mask, up, down, out,
    sv, gv, w1, w2, near, hop, far, last,
    sb0, sb1, sb2, sb3, sb4, xb0, xb1, xb2, xb3, xb4,
    ob0, ob1, ob2, ob3, ob4, rb0, rb1, rb2, rb3, rb4,
    zs, zr, posb, rowb, pick, pickr, cols, lpart, lrecv, fac, act, acc, hid,
    wsem, ssem, hsend, hrecv, isend, irecv, rsend, rrecv, zsend, zrecv, msend, mrecv,
):
    sb, xb = (sb0, sb1, sb2, sb3, sb4), (xb0, xb1, xb2, xb3, xb4)
    ob, rb = (ob0, ob1, ob2, ob3, ob4), (rb0, rb1, rb2, rb3, rb4)
    width = (16, 24, 24, 24, 16)
    ne = lax.axis_index("expert")
    x = lax.axis_index("gate")
    y, z, c = ne // (Z * C), (ne // C) % Z, ne % C
    half = Y * C * X * CAP // 2
    nf = sv.shape[0]
    rows = sv.shape[1]
    wide = sv.shape[2]
    share = rows // X

    def up_z(d):
        return lax.rem(z + d % Z, Z)

    def at_z(d):
        return (y * Z + up_z(d)) * C + c, x

    peers = Y * C * X

    def to_plane(visit):
        def one(i, k):
            dc, dx = k % C, k // C
            y2, c2, x2 = lax.rem(y + dx + i, Y), lax.rem(c + dc, C), lax.rem(x + dx, X)
            visit(y2, c2, x2, ((y2 * Z + z) * C + c2, x2))

        def some(i, carry):
            for k in range(C * X):
                one(i, k)
            return carry

        for k in range(1, C * X):
            one(0, k)
        lax.fori_loop(1, Y, some, 0)

    mine = (y * C + c) * X + x
    source = x * (Y * C) + y * C + c

    def remote(src, dst, ss, rs, dev):
        return pltpu.make_async_remote_copy(
            src_ref=src, dst_ref=dst, send_sem=ss, recv_sem=rs, device_id=dev, device_id_type=MESH
        )

    barrier = pltpu.get_barrier_semaphore()
    for d in (4, 3, 5, 2, 6, 1, 7):
        pl.semaphore_signal(barrier, inc=1, device_id=at_z(d), device_id_type=MESH)
    to_plane(lambda y2, c2, x2, dev: pl.semaphore_signal(barrier, inc=1, device_id=dev, device_id_type=MESH))

    def local(src, dst, sem):
        return pltpu.make_async_copy(src, dst, sem)

    fetch_s = [local(samples.at[:, pl.ds(f * wide, wide)], sv.at[f], ssem.at[f]) for f in range(nf)]
    for copy in fetch_s:
        copy.start()
    fetch_g = local(gate, gv, wsem.at[0])
    fetch_g.start()
    nt = w1.shape[0]
    hw, ow = w1.shape[4], w2.shape[2]
    fetch_1 = [
        local(up.at[xs, :, :, pl.ds(j * hw, hw)], w1.at[j, :, xs], wsem.at[1 + j * X + xs])
        for j in range(nt)
        for xs in range(X)
    ]
    fetch_2 = [
        local(down.at[0, :, pl.ds(j * ow, ow)], w2.at[j], wsem.at[1 + nt * X + j]) for j in range(nt)
    ]
    for copy in fetch_1 + fetch_2:
        copy.start()

    with jax.named_scope("greet"):
        pl.semaphore_wait(barrier, peers - 1 + Z - 1)

    sign = (1, -1)

    def hop_copy(step, way, f):
        dev = at_z(sign[way])
        sems = hsend.at[way, step, f], hrecv.at[way, step, f]
        if step == 0:
            src, dst = sv.at[f], near.at[way, 0, f]
        elif step == 1:
            src, dst = near.at[way, 0, f], near.at[way, 1, f]
        elif step == 2:
            src, dst = hop.at[way, f], far.at[way, f]
        else:
            src, dst = far.at[way, f, pl.ds(0, half)], last.at[way, f]
        return remote(src, dst, *sems, dev)

    for f in range(nf):
        fetch_s[f].wait()
        if f == 0:
            hop_copy(0, 0, 0).start()
            hop_copy(0, 1, 0).start()

    experts = gate.shape[1]
    earlier = as_mask(iota((rows, rows), 0) < iota((rows, rows), 1))
    named = [as_mask(iota((experts, rows), 0) == ids[k : k + 1, :]) for k in range(2)]
    count = jnp.dot((named[0].astype(F32) + named[1].astype(F32)).astype(BF16), earlier, **EXACT)
    rowb[...] = jnp.zeros_like(rowb)
    for k in range(2):
        rank = jnp.sum(named[k].astype(F32) * count, axis=0, keepdims=True)
        posb[0, k : k + 1, :] = ids[k : k + 1, :] * CAP + rank.astype(I32)
        rowb[k : k + 1, :] = ids[k : k + 1, :].astype(F32)
        rowb[2 + k : 3 + k, :] = rank
    rowb[4:5, :] = mask[...].reshape(1, rows).astype(F32)

    def pos_copy(d):
        return remote(posb.at[0], posb.at[d], msend.at[0], mrecv.at[0], at_z(d))

    for d in range(1, Z):
        pos_copy(d).start()
    for f in range(1, nf):
        hop_copy(0, 0, f).start()
        hop_copy(0, 1, f).start()

    same = as_mask(iota((rows, rows), 0) == iota((rows, rows), 1))
    turned = lax.dot_general(same, rowb[...].astype(BF16), (((1,), (1,)), ((), ())), **EXACT)
    cols[...] = turned.reshape(cols.shape)

    def target(shape, dim, n, a, plane):
        i = iota(shape, dim)
        if n == CAP:
            block, j = div(i, CAP * C * X), i
            return block * (Z * C * X * CAP - C * X * CAP) + plane * (C * X * CAP) + j
        d = div(i, n)
        s = i - d * n - a * CAP
        block = lax.shift_right_logical(d, 3)
        slot = block * (Z * C * X * CAP) + plane * (C * X * CAP) + (d - block * (C * X)) * CAP + s
        return jnp.where((s >= 0) & (s < CAP), slot, -1)

    def chooser(slots, d):
        p0, p1 = posb[d, 0:1, :], posb[d, 1:2, :]
        return as_mask((slots == p0) | (slots == p1))

    def put(g, f, value):
        sb[g][f] = value.reshape(peers, width[g], wide).astype(BF16)

    def send_in_plane(g, f):
        def one(y2, c2, x2, dev):
            to = (y2 * C + c2) * X + x2
            remote(sb[g].at[f, to], xb[g].at[f, source], isend.at[g, f], irecv.at[g, f], dev).start()

        to_plane(one)
        xb[g][f, source] = sb[g][f, mine]

    def dispatched(g, f):
        part = xb[g].at[f, pl.ds(0, peers - 1)]
        return remote(part, part, isend.at[g, f], irecv.at[g, f], along_x(1))

    def along_x(d):
        return ne, lax.rem(x + d, X)

    pick[0, : peers * 16, :] = chooser(target((peers * 16, 1), 0, 16, 0, z), 0)
    for f in range(nf):
        put(0, f, jnp.dot(pick[0, : peers * 16, :], sv[f], **EXACT))
        send_in_plane(0, f)

    fetch_g.wait()
    logits = jnp.zeros((rows, experts), F32)
    for f in range(nf):
        logits = logits + jnp.dot(sv[f], gv[f * wide : (f + 1) * wide, :], **EXACT)
    lpart[...] = logits.reshape(lpart.shape)

    def logit_copy(d):
        return remote(lpart.at[lax.rem(x + d, X)], lrecv.at[d - 1], msend.at[1], mrecv.at[1], along_x(d))

    for d in range(1, X):
        logit_copy(d).start()

    m_of = [Y * C * n for n in width]

    def features(g, f):
        part = [xb[g][f, xs * Y * C : (xs + 1) * Y * C].reshape(m_of[g], wide) for xs in range(X)]
        return jnp.concatenate(part, axis=1)

    def layer_1(g, f, j):
        return jnp.dot(features(g, f), w1[j, f].reshape(X * wide, hw), **EXACT)

    def partly(g, f):
        m = m_of[g]
        dispatched(g, f).wait_recv()

        def one(j, carry):
            if f == 0:
                hid[g - 3, j, 0:m, :] = layer_1(g, f, j)
            else:
                hid[g - 3, j, 0:m, :] += layer_1(g, f, j)
            return carry

        lax.fori_loop(0, nt, one, 0)

    def outward(g):
        n, m = width[g], m_of[g]

        def second(j, carry):
            whole = jnp.concatenate([act[i, 0:m, :] for i in range(nt)], axis=1)
            total = jnp.dot(whole, w2[j], **EXACT)
            ob[g][j] = total.reshape(Y * C, n, ow).astype(BF16)
            return carry

        lax.fori_loop(0, nt, second, 0)

        def one(y2, c2, x2, dev):
            remote(ob[g].at[x2, y2 * C + c2], rb[g].at[mine], rsend.at[g], rrecv.at[g], dev).start()

        to_plane(one)
        rb[g][mine] = ob[g][x, y * C + c]

    def expert(g):
        m = m_of[g]
        for f in range(nf):
            dispatched(g, f).wait_recv()

        def first(j, carry):
            total = layer_1(g, 0, j)
            for f in range(1, nf):
                total = total + layer_1(g, f, j)
            act[j, 0:m, :] = jnp.maximum(total, 0.0).astype(BF16)
            return carry

        lax.fori_loop(0, nt, first, 0)
        outward(g)

    def finish(g):
        m = m_of[g]
        partly(g, nf - 1)

        def first(j, carry):
            act[j, 0:m, :] = jnp.maximum(hid[g - 3, j, 0:m, :], 0.0).astype(BF16)
            return carry

        lax.fori_loop(0, nt, first, 0)
        outward(g)

    def back_in_plane(g):
        block = rb[g].at[pl.ds(0, peers - 1)]
        remote(block, block, rsend.at[g], rrecv.at[g], along_x(1)).wait_recv()

    def back_copy(d):
        return remote(zs.at[d], zr.at[d], zsend.at[d], zrecv.at[d], at_z(-d))

    def send_back(g, sources):
        n = width[g]
        q, i = iota((2 * half, peers * n), 0), iota((2 * half, peers * n), 1)
        base = q + div(q, CAP) * (n - CAP)
        got = rb[g][...].reshape(peers * n, rb[g].shape[2])
        for a, d in enumerate(sources):
            zs[d] = jnp.dot(as_mask(i == base + a * CAP), got, **EXACT).astype(BF16)
            back_copy(d).start()

    def add_up(plane, n, values, fresh=False):
        slots = target((1, values.shape[0]), 1, n, 0, plane)
        for k in range(2):
            col = cols[...].reshape(rows, 8)
            p = (col[:, k : k + 1] * CAP + col[:, 2 + k : 3 + k]).astype(I32)
            term = jnp.dot(as_mask(p == slots), values, **EXACT)
            if fresh:
                acc[k] = term
            else:
                acc[k] += term

    remote(posb.at[pl.ds(0, Z - 1)], posb.at[pl.ds(0, Z - 1)], msend.at[0], mrecv.at[0], along_x(1)).wait_recv()

    def choose_pair(g, dist):
        n = width[g]
        for a, d in enumerate((dist, Z - dist)):
            pick[a] = chooser(target((peers * n, 1), 0, n, a, z), d)

    def put_pair(g, dist, f):
        put(
            g, f,
            jnp.dot(pick[0], near[0, dist - 1, f], **EXACT) + jnp.dot(pick[1], near[1, dist - 1, f], **EXACT),
        )
        send_in_plane(g, f)

    def first_hop(f):
        for way in range(2):
            hop_copy(0, way, f).wait_recv()
            hop_copy(1, way, f).start()
        put_pair(1, 1, f)

    def second_hop(f):
        for way in range(2):
            hop_copy(1, way, f).wait_recv()
            hop[way, f] = jnp.dot(pickr[way], near[way, 1, f], **EXACT).astype(BF16)
            hop_copy(2, way, f).start()
        put_pair(2, 2, f)

    def spread(n, a, count):
        i, q = iota((count // CAP * n, count), 0), iota((count // CAP * n, count), 1)
        return as_mask(i == q + div(q, CAP) * (n - CAP) + a * CAP)

    def third_hop(f):
        for way in range(2):
            hop_copy(2, way, f).wait_recv()
            hop_copy(3, way, f).start()
        put(
            3, f,
            jnp.dot(pick[0, :, 0 : 2 * half], far[0, f, half:], **EXACT)
            + jnp.dot(pick[1, :, 0 : 2 * half], far[1, f, half:], **EXACT),
        )
        send_in_plane(3, f)

    def fourth_hop(f):
        half_peers = peers // 2
        grow = pick[0, 0 : half_peers * 16, 2 * half : 3 * half]
        for way in range(2):
            hop_copy(3, way, f).wait_recv()
            sb[4][f, way * half_peers : (way + 1) * half_peers] = (
                jnp.dot(grow, last[way, f], **EXACT).reshape(half_peers, 16, wide).astype(BF16)
            )
        send_in_plane(4, f)

    choose_pair(1, 1)
    first_hop(0)
    first_hop(1)
    for copy in fetch_1 + fetch_2:
        copy.wait()
    expert(0)
    first_hop(2)

    for way in range(2):
        d = 2 if way == 0 else Z - 2
        p3, p4 = up_z(sign[way]), up_z(2 * sign[way])
        q4 = target((2 * half, 1), 0, CAP, 0, p4)
        pickr[way, 0:half, :] = chooser(q4[way * half : (way + 1) * half], d)
        pickr[way, half:, :] = chooser(target((2 * half, 1), 0, CAP, 0, p3), d)

    remote(lrecv, lrecv, msend.at[1], mrecv.at[1], along_x(1)).wait_recv()
    logit = lpart[x] + lrecv[0] + lrecv[1] + lrecv[2]
    row_top = jnp.max(logit, axis=1, keepdims=True)
    term = jnp.exp(logit - row_top)
    row_total = jnp.sum(term, axis=1, keepdims=True)
    col = cols[x]
    lane = iota((share, experts), 1)
    both = []
    for k in range(2):
        chosen = jnp.sum(jnp.where(lane == col[:, k : k + 1].astype(I32), term, 0.0), axis=1, keepdims=True)
        both.append(experts * chosen / row_total * col[:, 4:5])
    wide_lane = iota((share, fac.shape[2]), 1)
    fac[x] = jnp.where(wide_lane == 0, both[0], jnp.where(wide_lane == 1, both[1], 0.0))

    def factor_copy(d):
        return remote(fac.at[x], fac.at[x], msend.at[2], mrecv.at[2], along_x(d))

    for d in range(1, X):
        factor_copy(d).start()

    back_in_plane(0)
    add_up(z, 16, rb[0][...].reshape(peers * 16, rb[0].shape[2]), True)

    def gather_back(d):
        back_copy(d).wait_recv()
        add_up(up_z(d), CAP, zr[d])

    first_hop(3)
    choose_pair(2, 2)
    second_hop(0)
    expert(1)
    second_hop(1)
    back_in_plane(1)
    send_back(1, (1, Z - 1))
    second_hop(2)
    second_hop(3)
    for a in range(2):
        pick[a, :, 0 : 2 * half] = spread(24, a, 2 * half)
    pick[0, 0 : peers * 8, 2 * half : 3 * half] = spread(16, 0, half)
    third_hop(0)
    expert(2)
    third_hop(1)
    gather_back(1)
    partly(3, 0)
    third_hop(2)
    partly(3, 1)
    back_in_plane(2)
    third_hop(3)
    send_back(2, (2, Z - 2))
    partly(3, 2)
    fourth_hop(0)
    fourth_hop(1)
    finish(3)
    fourth_hop(2)
    fourth_hop(3)
    partly(4, 0)
    partly(4, 1)
    back_in_plane(3)
    send_back(3, (3, Z - 3))
    partly(4, 2)
    finish(4)
    back_in_plane(4)
    send_back(4, (4,))
    for d in (7, 2, 6, 3, 5, 4):
        gather_back(d)

    block = fac.at[pl.ds(0, X - 1)]
    remote(block, block, msend.at[2], mrecv.at[2], along_x(1)).wait_recv()
    scale = fac[...].reshape(rows, fac.shape[2])
    out[...] = (scale[:, 0:1] * acc[0] + scale[:, 1:2] * acc[1]).astype(out.dtype)

    for step in range(4):
        for way in range(2):
            for f in range(nf):
                hop_copy(step, way, f).wait_send()
    remote(posb.at[pl.ds(0, Z - 1)], posb.at[pl.ds(0, Z - 1)], msend.at[0], mrecv.at[0], along_x(1)).wait_send()
    remote(lrecv, lrecv, msend.at[1], mrecv.at[1], along_x(1)).wait_send()
    remote(block, block, msend.at[2], mrecv.at[2], along_x(1)).wait_send()
    for g in range(5):
        for f in range(nf):
            dispatched(g, f).wait_send()
        sent = rb[g].at[pl.ds(0, peers - 1)]
        remote(sent, sent, rsend.at[g], rrecv.at[g], along_x(1)).wait_send()
    for d in range(1, Z):
        back_copy(d).wait_send()


def per_device(samples, gate_weight, expert_ids, pad_mask, up_weight, down_weight):
    rows, share = samples.shape
    experts = gate_weight.shape[1]
    depth, hidden = up_weight.shape[1:]
    columns = down_weight.shape[2] // X
    peers = Y * C * X
    nf = 4
    wide = share // nf
    width = (16, 24, 24, 24, 16)
    slots = peers * CAP
    dma = pltpu.SemaphoreType.DMA
    any_space = pl.BlockSpec(memory_space=pl.ANY)
    vmem = pl.BlockSpec(memory_space=pltpu.VMEM)
    scratch = [
        pltpu.VMEM((nf, rows, wide), BF16),
        pltpu.VMEM(gate_weight.shape, BF16),
        pltpu.VMEM((4, nf, X, wide, hidden // 4), BF16),
        pltpu.VMEM((4, hidden, columns), BF16),
        pltpu.VMEM((2, 2, nf, rows, wide), BF16),
        pltpu.VMEM((2, nf, slots * 3 // 2, wide), BF16),
        pltpu.VMEM((2, nf, slots * 3 // 2, wide), BF16),
        pltpu.VMEM((2, nf, slots // 2, wide), BF16),
    ]
    scratch += [pltpu.VMEM((nf, peers, n, wide), BF16) for n in width]
    scratch += [pltpu.VMEM((nf, peers, n, wide), BF16) for n in width]
    scratch += [pltpu.VMEM((X, Y * C, n, columns), BF16) for n in width]
    scratch += [pltpu.VMEM((peers, n, columns), BF16) for n in width]
    scratch += [
        pltpu.VMEM((Z, slots, columns), BF16),
        pltpu.VMEM((Z, slots, columns), BF16),
        pltpu.VMEM((Z, 2, rows), I32),
        pltpu.VMEM((8, rows), F32),
        pltpu.VMEM((2, peers * 24, rows), BF16),
        pltpu.VMEM((2, slots * 3 // 2, rows), BF16),
        pltpu.VMEM((X, rows // X, 8), F32),
        pltpu.VMEM((X, rows // X, experts), F32),
        pltpu.VMEM((X - 1, rows // X, experts), F32),
        pltpu.VMEM((X, rows // X, 128), F32),
        pltpu.VMEM((4, Y * C * 24, hidden // 4), BF16),
        pltpu.VMEM((2, rows, columns), F32),
        pltpu.VMEM((2, 4, Y * C * 24, hidden // 4), F32),
    ]
    scratch += [
        dma((5 + 4 * X,)), dma((nf,)), dma((2, 4, nf)), dma((2, 4, nf)), dma((5, nf)), dma((5, nf)),
        dma((5,)), dma((5,)), dma((Z,)), dma((Z,)), dma((3,)), dma((3,)),
    ]
    return pl.pallas_call(
        kernel,
        out_shape=jax.ShapeDtypeStruct((rows, columns), BF16),
        in_specs=[any_space, any_space, vmem, vmem, any_space, any_space],
        out_specs=vmem,
        scratch_shapes=scratch,
        compiler_params=pltpu.CompilerParams(
            collective_id=0, has_side_effects=True, vmem_limit_bytes=67043328
        ),
    )(samples, gate_weight, expert_ids.T, pad_mask,
      up_weight.reshape(X, nf, wide, hidden), down_weight)


def solution(mesh):
    placed = (
        P("expert", "gate"),
        P("gate", None),
        P("expert", None),
        P("expert"),
        P(("expert", "gate"), None, None),
        P(("expert", "gate"), None, None),
    )
    return jax.shard_map(
        per_device, mesh=mesh, in_specs=placed, out_specs=P("expert", "gate"), check_vma=False
    )
```

```python
import jax
import jax.numpy as jnp
from jax import lax
from jax.experimental import pallas as pl
from jax.experimental.pallas import tpu as pltpu
from jax.sharding import PartitionSpec as P

MESH = pl.DeviceIdType.MESH
Y, Z, C, X = 4, 8, 2, 4
CAP = 12
F32, BF16, I32 = jnp.float32, jnp.bfloat16, jnp.int32
EXACT = dict(preferred_element_type=F32)


def iota(shape, dim):
    return lax.broadcasted_iota(I32, shape, dim)


def div(v, n):
    return lax.shift_right_logical(v * (-(-(1 << 17) // n)), 17)


def as_mask(cond):
    return jnp.where(cond, 1.0, 0.0).astype(BF16)


def kernel(
    samples, gate, ids, mask, up, down, out,
    sv, gv, w1, w2, near, hop, far, last,
    sb0, sb1, sb2, sb3, sb4, xb0, xb1, xb2, xb3, xb4,
    ob0, ob1, ob2, ob3, ob4, rb0, rb1, rb2, rb3, rb4,
    zs, zr, posb, rowb, pick, pickr, cols, lpart, lrecv, fac, act, acc, hid, apart,
    wsem, ssem, known, hsend, hrecv, isend, irecv, rsend, rrecv, zsend, zrecv, msend, mrecv,
):
    sb, xb = (sb0, sb1, sb2, sb3, sb4), (xb0, xb1, xb2, xb3, xb4)
    ob, rb = (ob0, ob1, ob2, ob3, ob4), (rb0, rb1, rb2, rb3, rb4)
    width = (16, 24, 24, 24, 16)
    ne = lax.axis_index("expert")
    x = lax.axis_index("gate")
    y, z, c = ne // (Z * C), (ne // C) % Z, ne % C
    half = Y * C * X * CAP // 2
    nf = sv.shape[0]
    rows = sv.shape[1]
    wide = sv.shape[2]
    share = rows // X

    def up_z(d):
        return lax.rem(z + d % Z, Z)

    def at_z(d):
        return (y * Z + up_z(d)) * C + c, x

    peers = Y * C * X

    def to_plane(visit):
        def one(i, k):
            dc, dx = k % C, k // C
            y2, c2, x2 = lax.rem(y + dx + i, Y), lax.rem(c + dc, C), lax.rem(x + dx, X)
            visit(y2, c2, x2, ((y2 * Z + z) * C + c2, x2))

        def some(i, carry):
            for k in range(C * X):
                one(i, k)
            return carry

        for k in range(1, C * X):
            one(0, k)
        lax.fori_loop(1, Y, some, 0)

    mine = (y * C + c) * X + x
    source = x * (Y * C) + y * C + c

    def remote(src, dst, ss, rs, dev):
        return pltpu.make_async_remote_copy(
            src_ref=src, dst_ref=dst, send_sem=ss, recv_sem=rs, device_id=dev, device_id_type=MESH
        )

    barrier = pltpu.get_barrier_semaphore()
    z_near = (at_z(1), at_z(-1))
    y_near = tuple(((lax.rem(y + d, Y) * Z + z) * C + c, x) for d in (1, Y - 1))
    x_near = tuple((ne, lax.rem(x + d, X)) for d in (1, X - 1))
    partner = (((y * Z + z) * C + lax.rem(c + 1, C), x),)
    neighbours = z_near + y_near + x_near + partner
    for dev in neighbours:
        pl.semaphore_signal(barrier, inc=1, device_id=dev, device_id_type=MESH)

    def tell(i, devices):
        for dev in devices:
            pl.semaphore_signal(known.at[i], inc=1, device_id=dev, device_id_type=MESH)

    def heard(i, devices):
        pl.semaphore_wait(known.at[i], len(devices))

    def local(src, dst, sem):
        return pltpu.make_async_copy(src, dst, sem)

    fetch_s = [local(samples.at[:, pl.ds(f * wide, wide)], sv.at[f], ssem.at[f]) for f in range(nf)]
    for copy in fetch_s:
        copy.start()
    fetch_g = local(gate, gv, wsem.at[0])
    fetch_g.start()
    nt = w1.shape[0]
    hw, ow = w1.shape[4], w2.shape[2]
    fetch_1 = [
        local(up.at[xs, :, :, pl.ds(j * hw, hw)], w1.at[j, :, xs], wsem.at[1])
        for j in range(nt)
        for xs in range(X)
    ]
    fetch_2 = [
        local(down.at[0, :, pl.ds(j * ow, ow)], w2.at[j], wsem.at[2]) for j in range(nt)
    ]
    for copy in fetch_1 + fetch_2:
        copy.start()

    with jax.named_scope("greet"):
        pl.semaphore_wait(barrier, len(neighbours))

    sign = (1, -1)

    def hop_copy(step, way, f):
        dev = at_z(sign[way])
        sems = hsend.at[step], hrecv.at[way, step, f]
        if step == 0:
            src, dst = sv.at[f], near.at[way, 0, f]
        elif step == 1:
            src, dst = near.at[way, 0, f], near.at[way, 1, f]
        elif step == 2:
            src, dst = hop.at[way, f], far.at[way, f]
        else:
            src, dst = far.at[way, f, pl.ds(0, half)], last.at[way, f]
        return remote(src, dst, *sems, dev)

    for f in range(nf):
        fetch_s[f].wait()
        if f == 0:
            hop_copy(0, 0, 0).start()
            hop_copy(0, 1, 0).start()
            tell(0, x_near)
            tell(1, z_near)

    experts = gate.shape[1]
    earlier = as_mask(iota((rows, rows), 0) < iota((rows, rows), 1))
    named = [as_mask(iota((experts, rows), 0) == ids[k : k + 1, :]) for k in range(2)]
    count = jnp.dot((named[0].astype(F32) + named[1].astype(F32)).astype(BF16), earlier, **EXACT)
    rowb[...] = jnp.zeros_like(rowb)
    for k in range(2):
        rank = jnp.sum(named[k].astype(F32) * count, axis=0, keepdims=True)
        posb[0, k : k + 1, :] = ids[k : k + 1, :] * CAP + rank.astype(I32)
        rowb[k : k + 1, :] = ids[k : k + 1, :].astype(F32)
        rowb[2 + k : 3 + k, :] = rank
    rowb[4:5, :] = mask[...].reshape(1, rows).astype(F32)

    def pos_copy(d):
        return remote(posb.at[0], posb.at[d], msend.at[0], mrecv.at[0], at_z(d))

    heard(1, z_near)
    tell(2, z_near)
    heard(0, x_near)
    tell(3, y_near)
    near_z = (1, Z - 1, 2, Z - 2)
    for d in near_z:
        pos_copy(d).start()
    for f in range(1, nf):
        hop_copy(0, 0, f).start()
        hop_copy(0, 1, f).start()

    same = as_mask(iota((rows, rows), 0) == iota((rows, rows), 1))
    turned = lax.dot_general(same, rowb[...].astype(BF16), (((1,), (1,)), ((), ())), **EXACT)
    cols[...] = turned.reshape(cols.shape)
    heard(3, y_near)
    tell(4, y_near)
    heard(2, z_near)
    tell(5, z_near)

    def target(shape, dim, n, a, plane):
        i = iota(shape, dim)
        if n == CAP:
            block, j = div(i, CAP * C * X), i
            return block * (Z * C * X * CAP - C * X * CAP) + plane * (C * X * CAP) + j
        d = div(i, n)
        s = i - d * n - a * CAP
        block = lax.shift_right_logical(d, 3)
        slot = block * (Z * C * X * CAP) + plane * (C * X * CAP) + (d - block * (C * X)) * CAP + s
        return jnp.where((s >= 0) & (s < CAP), slot, -1)

    def chooser(slots, d):
        p0, p1 = posb[d, 0:1, :], posb[d, 1:2, :]
        return as_mask((slots == p0) | (slots == p1))

    def put(g, f, value):
        sb[g][f] = value.reshape(peers, width[g], wide).astype(BF16)

    def send_in_plane(g, f):
        def one(y2, c2, x2, dev):
            to = (y2 * C + c2) * X + x2
            remote(sb[g].at[f, to], xb[g].at[f, source], isend.at[g], irecv.at[g, f], dev).start()

        to_plane(one)
        xb[g][f, source] = sb[g][f, mine]

    def dispatched(g, f):
        part = xb[g].at[f, pl.ds(0, peers - 1)]
        return remote(part, part, isend.at[g], irecv.at[g, f], along_x(1))

    def along_x(d):
        return ne, lax.rem(x + d, X)

    fetch_g.wait()
    logits = jnp.zeros((rows, experts), F32)
    for f in range(nf):
        logits = logits + jnp.dot(sv[f], gv[f * wide : (f + 1) * wide, :], **EXACT)
    lpart[...] = logits.reshape(lpart.shape)

    def logit_copy(d):
        return remote(lpart.at[lax.rem(x + d, X)], lrecv.at[d - 1], msend.at[1], mrecv.at[1], along_x(d))

    for d in range(1, X):
        logit_copy(d).start()

    heard(4, y_near)
    tell(6, partner)
    heard(5, z_near)
    pick[0, : peers * 16, :] = chooser(target((peers * 16, 1), 0, 16, 0, z), 0)
    for f in range(nf):
        put(0, f, jnp.dot(pick[0, : peers * 16, :], sv[f], **EXACT))
        if f == 0:
            heard(6, partner)
        send_in_plane(0, f)

    m_of = [Y * C * n for n in width]

    def features(g, f):
        part = [xb[g][f, xs * Y * C : (xs + 1) * Y * C].reshape(m_of[g], wide) for xs in range(X)]
        return jnp.concatenate(part, axis=1)

    def layer_1(g, f, j):
        part = features(g, f) if g < 4 else apart[...]
        return jnp.dot(part, w1[j, f].reshape(X * wide, hw), **EXACT)

    def partly(g, f):
        m = m_of[g]
        if g < 4:
            dispatched(g, f).wait_recv()
        else:
            h, a = f // 2, f % 2
            if a == 0:
                dispatched(g, h).wait_recv()
            i, r = iota((m, Y * C * 24), 1), iota((m, Y * C * 24), 0)
            p = lax.shift_right_logical(r, 4)
            keep = (i == p * 24 + (r - p * 16) + a * CAP) & (r - p * 16 < CAP)
            both = [xb[g][h, xs * Y * C : (xs + 1) * Y * C].reshape(Y * C * 24, wide) for xs in range(X)]
            for xs in range(X):
                part = jnp.dot(as_mask(keep), both[xs], **EXACT)
                apart[:, xs * wide : (xs + 1) * wide] = part.astype(BF16)

        def one(j, carry):
            if f == 0:
                hid[g - 3, j, 0:m, :] = layer_1(g, f, j)
            else:
                hid[g - 3, j, 0:m, :] += layer_1(g, f, j)
            return carry

        lax.fori_loop(0, nt, one, 0)

    def outward(g):
        n, m = width[g], m_of[g]
        for dx in (2, 1, 3, 0):
            x2 = lax.rem(x + dx, X)
            whole = jnp.concatenate([act[i, 0:m, :] for i in range(nt)], axis=1)
            total = jnp.dot(whole, w2[x2], **EXACT)
            ob[g][x2] = total.reshape(Y * C, n, ow).astype(BF16)
            for dy in (2, 1, 3, 0):
                for dc in range(C):
                    y2, c2 = lax.rem(y + dy, Y), lax.rem(c + dc, C)
                    if dx + dy + dc:
                        dev = (y2 * Z + z) * C + c2, x2
                        remote(ob[g].at[x2, y2 * C + c2], rb[g].at[mine], rsend.at[g], rrecv.at[g], dev).start()
        rb[g][mine] = ob[g][x, y * C + c]

    def expert(g):
        m = m_of[g]
        for f in range(nf):
            dispatched(g, f).wait_recv()

        def first(j, carry):
            total = layer_1(g, 0, j)
            for f in range(1, nf):
                total = total + layer_1(g, f, j)
            act[j, 0:m, :] = jnp.maximum(total, 0.0).astype(BF16)
            return carry

        lax.fori_loop(0, nt, first, 0)
        outward(g)

    def finish(g):
        m = m_of[g]
        partly(g, nf - 1)

        def first(j, carry):
            act[j, 0:m, :] = jnp.maximum(hid[g - 3, j, 0:m, :], 0.0).astype(BF16)
            return carry

        lax.fori_loop(0, nt, first, 0)
        outward(g)

    def back_in_plane(g):
        block = rb[g].at[pl.ds(0, peers - 1)]
        remote(block, block, rsend.at[g], rrecv.at[g], along_x(1)).wait_recv()

    def back_copy(d):
        return remote(zs.at[d], zr.at[d], zsend.at[0], zrecv.at[d], at_z(-d))

    def send_back(g, sources):
        n = width[g]
        q, i = iota((2 * half, peers * n), 0), iota((2 * half, peers * n), 1)
        base = q + div(q, CAP) * (n - CAP)
        got = rb[g][...].reshape(peers * n, rb[g].shape[2])
        for a, d in enumerate(sources):
            zs[d] = jnp.dot(as_mask(i == base + a * CAP), got, **EXACT).astype(BF16)
            back_copy(d).start()

    def add_up(plane, n, values, fresh=False):
        slots = target((1, values.shape[0]), 1, n, 0, plane)
        for k in range(2):
            col = cols[...].reshape(rows, 8)
            p = (col[:, k : k + 1] * CAP + col[:, 2 + k : 3 + k]).astype(I32)
            term = jnp.dot(as_mask(p == slots), values, **EXACT)
            if fresh:
                acc[k] = term
            else:
                acc[k] += term

    shared = posb.at[pl.ds(0, len(near_z))]
    shared = remote(shared, shared, msend.at[0], mrecv.at[0], along_x(1))

    def choose_pair(g, dist):
        n = width[g]
        for a, d in enumerate((dist, Z - dist)):
            pick[a] = chooser(target((peers * n, 1), 0, n, a, z), d)

    def put_pair(g, dist, f):
        put(
            g, f,
            jnp.dot(pick[0], near[0, dist - 1, f], **EXACT) + jnp.dot(pick[1], near[1, dist - 1, f], **EXACT),
        )
        send_in_plane(g, f)

    def first_hop(f):
        for way in range(2):
            hop_copy(0, way, f).wait_recv()
            hop_copy(1, way, f).start()
        if f == 0:
            shared.wait_recv()
            choose_pair(1, 1)
        put_pair(1, 1, f)

    def second_hop(f):
        for way in range(2):
            hop_copy(1, way, f).wait_recv()
            hop[way, f] = jnp.dot(pickr[way], near[way, 1, f], **EXACT).astype(BF16)
            hop_copy(2, way, f).start()
        put_pair(2, 2, f)

    def spread(n, a, count):
        i, q = iota((count // CAP * n, count), 0), iota((count // CAP * n, count), 1)
        return as_mask(i == q + div(q, CAP) * (n - CAP) + a * CAP)

    def third_hop(f):
        for way in range(2):
            hop_copy(2, way, f).wait_recv()
            hop_copy(3, way, f).start()
        put(
            3, f,
            jnp.dot(pick[0, :, 0 : 2 * half], far[0, f, half:], **EXACT)
            + jnp.dot(pick[1, :, 0 : 2 * half], far[1, f, half:], **EXACT),
        )
        send_in_plane(3, f)

    def fourth_hop(h):
        half_peers = peers // 2
        for way in range(2):
            total = jnp.zeros((half_peers * 24, wide), F32)
            for a in range(2):
                hop_copy(3, way, 2 * h + a).wait_recv()
                total = total + jnp.dot(pick[a, 0 : half_peers * 24, 0:half], last[way, 2 * h + a], **EXACT)
            sb[4][h, way * half_peers : (way + 1) * half_peers] = (
                total.reshape(half_peers, 24, wide).astype(BF16)
            )
        send_in_plane(4, h)

    first_hop(0)
    first_hop(1)
    local(w1, w1, wsem.at[1]).wait()
    local(w2, w2, wsem.at[2]).wait()
    expert(0)
    first_hop(2)

    for way in range(2):
        d = 2 if way == 0 else Z - 2
        p3, p4 = up_z(sign[way]), up_z(2 * sign[way])
        q4 = target((2 * half, 1), 0, CAP, 0, p4)
        pickr[way, 0:half, :] = chooser(q4[way * half : (way + 1) * half], d)
        pickr[way, half:, :] = chooser(target((2 * half, 1), 0, CAP, 0, p3), d)

    remote(lrecv, lrecv, msend.at[1], mrecv.at[1], along_x(1)).wait_recv()
    logit = lpart[x] + lrecv[0] + lrecv[1] + lrecv[2]
    row_top = jnp.max(logit, axis=1, keepdims=True)
    term = jnp.exp(logit - row_top)
    row_total = jnp.sum(term, axis=1, keepdims=True)
    col = cols[x]
    lane = iota((share, experts), 1)
    both = []
    for k in range(2):
        chosen = jnp.sum(jnp.where(lane == col[:, k : k + 1].astype(I32), term, 0.0), axis=1, keepdims=True)
        both.append(experts * chosen / row_total * col[:, 4:5])
    wide_lane = iota((share, fac.shape[2]), 1)
    fac[x] = jnp.where(wide_lane == 0, both[0], jnp.where(wide_lane == 1, both[1], 0.0))

    def factor_copy(d):
        return remote(fac.at[x], fac.at[x], msend.at[2], mrecv.at[2], along_x(d))

    for d in range(1, X):
        factor_copy(d).start()

    back_in_plane(0)
    add_up(z, 16, rb[0][...].reshape(peers * 16, rb[0].shape[2]), True)

    def gather_back(d):
        back_copy(d).wait_recv()
        add_up(up_z(d), CAP, zr[d])

    first_hop(3)
    choose_pair(2, 2)
    second_hop(0)
    expert(1)
    second_hop(1)
    back_in_plane(1)
    send_back(1, (1, Z - 1))
    second_hop(2)
    second_hop(3)
    for a in range(2):
        pick[a, :, 0 : 2 * half] = spread(24, a, 2 * half)
    last_slots = target((1, 2 * half), 1, CAP, 0, up_z(4))
    for k in range(2):
        col = cols[...].reshape(rows, 8)
        p = (col[:, k : k + 1] * CAP + col[:, 2 + k : 3 + k]).astype(I32)
        pick[k, :, 2 * half : 4 * half] = as_mask(p == last_slots)
    third_hop(0)
    expert(2)
    third_hop(1)
    gather_back(1)
    partly(3, 0)
    third_hop(2)
    partly(3, 1)
    back_in_plane(2)
    third_hop(3)
    send_back(2, (2, Z - 2))
    partly(3, 2)
    fourth_hop(0)
    finish(3)
    fourth_hop(1)
    partly(4, 0)
    partly(4, 1)
    back_in_plane(3)
    send_back(3, (3, Z - 3))
    partly(4, 2)
    finish(4)
    back_in_plane(4)
    send_back(4, (4,))
    for d in (7, 2, 6, 3, 5):
        gather_back(d)

    block = fac.at[pl.ds(0, X - 1)]
    remote(block, block, msend.at[2], mrecv.at[2], along_x(1)).wait_recv()
    scale = fac[...].reshape(rows, fac.shape[2])
    for step, whole in enumerate((near.at[:, 0], near.at[:, 1], hop, last)):
        remote(whole, whole, hsend.at[step], hrecv.at[0, step, 0], at_z(1)).wait_send()
    shared.wait_send()
    remote(lrecv, lrecv, msend.at[1], mrecv.at[1], along_x(1)).wait_send()
    remote(block, block, msend.at[2], mrecv.at[2], along_x(1)).wait_send()
    for g in range(5):
        sent = xb[g].at[:, pl.ds(0, peers - 1)]
        remote(sent, sent, isend.at[g], irecv.at[g, 0], along_x(1)).wait_send()
        sent = rb[g].at[pl.ds(0, peers - 1)]
        remote(sent, sent, rsend.at[g], rrecv.at[g], along_x(1)).wait_send()
    sent = zs.at[pl.ds(1, Z - 1)]
    remote(sent, sent, zsend.at[0], zrecv.at[1], at_z(1)).wait_send()

    back_copy(4).wait_recv()
    final = [acc[k] + jnp.dot(pick[k, :, 2 * half : 4 * half], zr[4], **EXACT) for k in range(2)]
    out[...] = (scale[:, 0:1] * final[0] + scale[:, 1:2] * final[1]).astype(out.dtype)


def per_device(samples, gate_weight, expert_ids, pad_mask, up_weight, down_weight):
    rows, share = samples.shape
    experts = gate_weight.shape[1]
    depth, hidden = up_weight.shape[1:]
    columns = down_weight.shape[2] // X
    peers = Y * C * X
    nf = 4
    wide = share // nf
    width = (16, 24, 24, 24, 16)
    slots = peers * CAP
    dma = pltpu.SemaphoreType.DMA
    any_space = pl.BlockSpec(memory_space=pl.ANY)
    vmem = pl.BlockSpec(memory_space=pltpu.VMEM)
    scratch = [
        pltpu.VMEM((nf, rows, wide), BF16),
        pltpu.VMEM(gate_weight.shape, BF16),
        pltpu.VMEM((4, nf, X, wide, hidden // 4), BF16),
        pltpu.VMEM((4, hidden, columns), BF16),
        pltpu.VMEM((2, 2, nf, rows, wide), BF16),
        pltpu.VMEM((2, nf, slots * 3 // 2, wide), BF16),
        pltpu.VMEM((2, nf, slots * 3 // 2, wide), BF16),
        pltpu.VMEM((2, nf, slots // 2, wide), BF16),
    ]
    messages = [(nf, peers, n, wide) for n in width[:4]] + [(nf // 2, peers, 24, wide)]
    scratch += [pltpu.VMEM(shape, BF16) for shape in messages * 2]
    scratch += [pltpu.VMEM((X, Y * C, n, columns), BF16) for n in width]
    scratch += [pltpu.VMEM((peers, n, columns), BF16) for n in width]
    scratch += [
        pltpu.VMEM((Z, slots, columns), BF16),
        pltpu.VMEM((Z, slots, columns), BF16),
        pltpu.VMEM((Z, 2, rows), I32),
        pltpu.VMEM((8, rows), F32),
        pltpu.VMEM((2, peers * 24, rows), BF16),
        pltpu.VMEM((2, slots * 3 // 2, rows), BF16),
        pltpu.VMEM((X, rows // X, 8), F32),
        pltpu.VMEM((X, rows // X, experts), F32),
        pltpu.VMEM((X - 1, rows // X, experts), F32),
        pltpu.VMEM((X, rows // X, 128), F32),
        pltpu.VMEM((4, Y * C * 24, hidden // 4), BF16),
        pltpu.VMEM((2, rows, columns), F32),
        pltpu.VMEM((2, 4, Y * C * 24, hidden // 4), F32),
        pltpu.VMEM((Y * C * 16, depth // 4), BF16),
    ]
    scratch += [
        dma((3,)), dma((nf,)), pltpu.SemaphoreType.REGULAR((7,)), dma((4,)), dma((2, 4, nf)), dma((5,)), dma((5, nf)),
        dma((5,)), dma((5,)), dma((1,)), dma((Z,)), dma((3,)), dma((3,)),
    ]
    return pl.pallas_call(
        kernel,
        out_shape=jax.ShapeDtypeStruct((rows, columns), BF16),
        in_specs=[any_space, any_space, vmem, vmem, any_space, any_space],
        out_specs=vmem,
        scratch_shapes=scratch,
        compiler_params=pltpu.CompilerParams(
            collective_id=0, has_side_effects=True, vmem_limit_bytes=67043328
        ),
    )(samples, gate_weight, expert_ids.T, pad_mask,
      up_weight.reshape(X, nf, wide, hidden), down_weight)


def solution(mesh):
    placed = (
        P("expert", "gate"),
        P("gate", None),
        P("expert", None),
        P("expert"),
        P(("expert", "gate"), None, None),
        P(("expert", "gate"), None, None),
    )
    return jax.shard_map(
        per_device, mesh=mesh, in_specs=placed, out_specs=P("expert", "gate"), check_vma=False
    )
```

```python
import jax
import jax.numpy as jnp
from jax import lax
from jax.experimental import pallas as pl
from jax.experimental.pallas import tpu as pltpu
from jax.sharding import PartitionSpec as P

MESH = pl.DeviceIdType.MESH
Y, Z, C, X = 4, 8, 2, 4
CAP = 12
F32, BF16, I32 = jnp.float32, jnp.bfloat16, jnp.int32
EXACT = dict(preferred_element_type=F32)


def iota(shape, dim):
    return lax.broadcasted_iota(I32, shape, dim)


def div(v, n):
    return lax.shift_right_logical(v * (-(-(1 << 17) // n)), 17)


def as_mask(cond):
    return jnp.where(cond, 1.0, 0.0).astype(BF16)


def kernel(
    samples, gate, ids, mask, up, down, out,
    sv, gv, w1, w2, near, hop, far, last,
    sb0, sb1, sb2, sb3, sb4, xb0, xb1, xb2, xb3, xb4,
    ob0, ob1, ob2, ob3, ob4, rb0, rb1, rb2, rb3, rb4,
    zs, zr, posb, rowb, pick, pickr, cols, lpart, lrecv, fac, act, acc, hid, apart,
    wsem, ssem, known, hsend, hrecv, isend, irecv, rsend, rrecv, zsend, zrecv, msend, mrecv,
):
    sb, xb = (sb0, sb1, sb2, sb3, sb4), (xb0, xb1, xb2, xb3, xb4)
    ob, rb = (ob0, ob1, ob2, ob3, ob4), (rb0, rb1, rb2, rb3, rb4)
    width = (16, 24, 24, 24, 16)
    ne = lax.axis_index("expert")
    x = lax.axis_index("gate")
    y, z, c = ne // (Z * C), (ne // C) % Z, ne % C
    half = Y * C * X * CAP // 2
    nf = sv.shape[0]
    rows = sv.shape[1]
    wide = sv.shape[2]
    share = rows // X

    def up_z(d):
        return lax.rem(z + d % Z, Z)

    def at_z(d):
        return (y * Z + up_z(d)) * C + c, x

    peers = Y * C * X

    def to_plane(visit):
        order = [(dx, dc) for dx in (2, 1, 3, 0) for dc in (1, 0)]

        def one(i, dx, dc):
            y2, c2, x2 = lax.rem(y + dx + i, Y), lax.rem(c + dc, C), lax.rem(x + dx, X)
            visit(y2, c2, x2, ((y2 * Z + z) * C + c2, x2))

        def some(i, carry):
            for dx, dc in order:
                one(i, dx, dc)
            return carry

        for dx, dc in order[:-1]:
            one(0, dx, dc)
        lax.fori_loop(1, Y, some, 0)

    mine = (y * C + c) * X + x
    source = x * (Y * C) + y * C + c

    def remote(src, dst, ss, rs, dev):
        return pltpu.make_async_remote_copy(
            src_ref=src, dst_ref=dst, send_sem=ss, recv_sem=rs, device_id=dev, device_id_type=MESH
        )

    barrier = pltpu.get_barrier_semaphore()
    z_near = (at_z(1), at_z(-1))
    y_near = tuple(((lax.rem(y + d, Y) * Z + z) * C + c, x) for d in (1, Y - 1))
    x_near = tuple((ne, lax.rem(x + d, X)) for d in (1, X - 1))
    partner = (((y * Z + z) * C + lax.rem(c + 1, C), x),)
    neighbours = z_near + y_near + x_near + partner
    for dev in neighbours:
        pl.semaphore_signal(barrier, inc=1, device_id=dev, device_id_type=MESH)

    def tell(i, devices):
        for dev in devices:
            pl.semaphore_signal(known.at[i], inc=1, device_id=dev, device_id_type=MESH)

    def heard(i, devices):
        pl.semaphore_wait(known.at[i], len(devices))

    def local(src, dst, sem):
        return pltpu.make_async_copy(src, dst, sem)

    fetch_s = [local(samples.at[:, pl.ds(f * wide, wide)], sv.at[f], ssem.at[f]) for f in range(nf)]
    for copy in fetch_s:
        copy.start()
    fetch_g = local(gate, gv, wsem.at[0])
    fetch_g.start()
    nt = w1.shape[0]
    hw, ow = w1.shape[4], w2.shape[2]
    fetch_1 = [
        local(up.at[xs, :, :, pl.ds(j * hw, hw)], w1.at[j, :, xs], wsem.at[1])
        for j in range(nt)
        for xs in range(X)
    ]
    fetch_2 = [
        local(down.at[0, :, pl.ds(j * ow, ow)], w2.at[j], wsem.at[2]) for j in range(nt)
    ]
    for copy in fetch_1 + fetch_2:
        copy.start()

    with jax.named_scope("greet"):
        pl.semaphore_wait(barrier, len(neighbours))

    sign = (1, -1)

    def hop_copy(step, way, f):
        dev = at_z(sign[way])
        sems = hsend.at[step], hrecv.at[way, step, f]
        if step == 0:
            src, dst = sv.at[f], near.at[way, 0, f]
        elif step == 1:
            src, dst = near.at[way, 0, f], near.at[way, 1, f]
        elif step == 2:
            src, dst = hop.at[way, f], far.at[way, f]
        else:
            src, dst = far.at[way, f, pl.ds(0, half)], last.at[way, f]
        return remote(src, dst, *sems, dev)

    for f in range(nf):
        fetch_s[f].wait()
        if f == 0:
            hop_copy(0, 0, 0).start()
            hop_copy(0, 1, 0).start()
            tell(0, x_near)
            tell(1, z_near)

    experts = gate.shape[1]
    earlier = as_mask(iota((rows, rows), 0) < iota((rows, rows), 1))
    named = [as_mask(iota((experts, rows), 0) == ids[k : k + 1, :]) for k in range(2)]
    count = jnp.dot((named[0].astype(F32) + named[1].astype(F32)).astype(BF16), earlier, **EXACT)
    rowb[...] = jnp.zeros_like(rowb)
    for k in range(2):
        rank = jnp.sum(named[k].astype(F32) * count, axis=0, keepdims=True)
        posb[0, k : k + 1, :] = ids[k : k + 1, :] * CAP + rank.astype(I32)
        rowb[k : k + 1, :] = ids[k : k + 1, :].astype(F32)
        rowb[2 + k : 3 + k, :] = rank
    rowb[4:5, :] = mask[...].reshape(1, rows).astype(F32)

    def pos_copy(d):
        return remote(posb.at[0], posb.at[d], msend.at[0], mrecv.at[0], at_z(d))

    heard(1, z_near)
    tell(2, z_near)
    heard(0, x_near)
    tell(3, y_near)
    near_z = (1, Z - 1, 2, Z - 2)
    for d in near_z:
        pos_copy(d).start()
    for f in range(1, nf):
        hop_copy(0, 0, f).start()
        hop_copy(0, 1, f).start()

    same = as_mask(iota((rows, rows), 0) == iota((rows, rows), 1))
    turned = lax.dot_general(same, rowb[...].astype(BF16), (((1,), (1,)), ((), ())), **EXACT)
    cols[...] = turned.reshape(cols.shape)
    heard(3, y_near)
    tell(4, y_near)
    heard(2, z_near)
    tell(5, z_near)

    def target(shape, dim, n, a, plane):
        i = iota(shape, dim)
        if n == CAP:
            block, j = div(i, CAP * C * X), i
            return block * (Z * C * X * CAP - C * X * CAP) + plane * (C * X * CAP) + j
        d = div(i, n)
        s = i - d * n - a * CAP
        block = lax.shift_right_logical(d, 3)
        slot = block * (Z * C * X * CAP) + plane * (C * X * CAP) + (d - block * (C * X)) * CAP + s
        return jnp.where((s >= 0) & (s < CAP), slot, -1)

    def chooser(slots, d):
        p0, p1 = posb[d, 0:1, :], posb[d, 1:2, :]
        return as_mask((slots == p0) | (slots == p1))

    def put(g, f, value):
        sb[g][f] = value.reshape(peers, width[g], wide).astype(BF16)

    def send_in_plane(g, f):
        def one(y2, c2, x2, dev):
            to = (y2 * C + c2) * X + x2
            remote(sb[g].at[f, to], xb[g].at[f, source], isend.at[g], irecv.at[g, f], dev).start()

        to_plane(one)
        xb[g][f, source] = sb[g][f, mine]

    def dispatched(g, f):
        part = xb[g].at[f, pl.ds(0, peers - 1)]
        return remote(part, part, isend.at[g], irecv.at[g, f], along_x(1))

    def along_x(d):
        return ne, lax.rem(x + d, X)

    fetch_g.wait()
    logits = jnp.zeros((rows, experts), F32)
    for f in range(nf):
        logits = logits + jnp.dot(sv[f], gv[f * wide : (f + 1) * wide, :], **EXACT)
    lpart[...] = logits.reshape(lpart.shape)

    def logit_copy(d):
        return remote(lpart.at[lax.rem(x + d, X)], lrecv.at[d - 1], msend.at[1], mrecv.at[1], along_x(d))

    for d in range(1, X):
        logit_copy(d).start()

    heard(4, y_near)
    tell(6, partner)
    heard(5, z_near)
    pick[0, : peers * 16, :] = chooser(target((peers * 16, 1), 0, 16, 0, z), 0)
    for f in range(nf):
        put(0, f, jnp.dot(pick[0, : peers * 16, :], sv[f], **EXACT))
        if f == 0:
            heard(6, partner)
        send_in_plane(0, f)

    m_of = [Y * C * n for n in width]

    def features(g, f):
        part = [xb[g][f, xs * Y * C : (xs + 1) * Y * C].reshape(m_of[g], wide) for xs in range(X)]
        return jnp.concatenate(part, axis=1)

    def layer_1(g, f, j):
        part = features(g, f) if g < 4 else apart[...]
        return jnp.dot(part, w1[j, f].reshape(X * wide, hw), **EXACT)

    def partly(g, f):
        m = m_of[g]
        if g < 4:
            dispatched(g, f).wait_recv()
        else:
            h, a = f // 2, f % 2
            if a == 0:
                dispatched(g, h).wait_recv()
            i, r = iota((m, Y * C * 24), 1), iota((m, Y * C * 24), 0)
            p = lax.shift_right_logical(r, 4)
            keep = (i == p * 24 + (r - p * 16) + a * CAP) & (r - p * 16 < CAP)
            both = [xb[g][h, xs * Y * C : (xs + 1) * Y * C].reshape(Y * C * 24, wide) for xs in range(X)]
            for xs in range(X):
                part = jnp.dot(as_mask(keep), both[xs], **EXACT)
                apart[:, xs * wide : (xs + 1) * wide] = part.astype(BF16)

        def one(j, carry):
            if f == 0:
                hid[g - 3, j, 0:m, :] = layer_1(g, f, j)
            else:
                hid[g - 3, j, 0:m, :] += layer_1(g, f, j)
            return carry

        lax.fori_loop(0, nt, one, 0)

    def outward(g):
        n, m = width[g], m_of[g]
        for dx in (2, 1, 3, 0):
            x2 = lax.rem(x + dx, X)
            whole = jnp.concatenate([act[i, 0:m, :] for i in range(nt)], axis=1)
            total = jnp.dot(whole, w2[x2], **EXACT)
            ob[g][x2] = total.reshape(Y * C, n, ow).astype(BF16)
            for dy in (2, 1, 3, 0):
                for dc in range(C):
                    y2, c2 = lax.rem(y + dy, Y), lax.rem(c + dc, C)
                    if dx + dy + dc:
                        dev = (y2 * Z + z) * C + c2, x2
                        remote(ob[g].at[x2, y2 * C + c2], rb[g].at[mine], rsend.at[g], rrecv.at[g], dev).start()
        rb[g][mine] = ob[g][x, y * C + c]

    def expert(g):
        m = m_of[g]
        for f in range(nf):
            dispatched(g, f).wait_recv()

        def first(j, carry):
            total = layer_1(g, 0, j)
            for f in range(1, nf):
                total = total + layer_1(g, f, j)
            act[j, 0:m, :] = jnp.maximum(total, 0.0).astype(BF16)
            return carry

        lax.fori_loop(0, nt, first, 0)
        outward(g)

    def finish(g):
        m = m_of[g]
        partly(g, nf - 1)

        def first(j, carry):
            act[j, 0:m, :] = jnp.maximum(hid[g - 3, j, 0:m, :], 0.0).astype(BF16)
            return carry

        lax.fori_loop(0, nt, first, 0)
        outward(g)

    def back_in_plane(g):
        block = rb[g].at[pl.ds(0, peers - 1)]
        remote(block, block, rsend.at[g], rrecv.at[g], along_x(1)).wait_recv()

    def back_copy(d):
        return remote(zs.at[d], zr.at[d], zsend.at[0], zrecv.at[d], at_z(-d))

    def sort_back(g, sources):
        n = width[g]
        q, i = iota((2 * half, peers * n), 0), iota((2 * half, peers * n), 1)
        base = q + div(q, CAP) * (n - CAP)
        got = rb[g][...].reshape(peers * n, rb[g].shape[2])
        for a, d in enumerate(sources):
            zs[d] = jnp.dot(as_mask(i == base + a * CAP), got, **EXACT).astype(BF16)
            if g > 2:
                back_copy(d).start()

    def add_up(plane, n, values, fresh=False):
        slots = target((1, values.shape[0]), 1, n, 0, plane)
        for k in range(2):
            col = cols[...].reshape(rows, 8)
            p = (col[:, k : k + 1] * CAP + col[:, 2 + k : 3 + k]).astype(I32)
            term = jnp.dot(as_mask(p == slots), values, **EXACT)
            if fresh:
                acc[k] = term
            else:
                acc[k] += term

    shared = posb.at[pl.ds(0, len(near_z))]
    shared = remote(shared, shared, msend.at[0], mrecv.at[0], along_x(1))

    def choose_pair(g, dist):
        n = width[g]
        for a, d in enumerate((dist, Z - dist)):
            pick[a] = chooser(target((peers * n, 1), 0, n, a, z), d)

    def put_pair(g, dist, f):
        put(
            g, f,
            jnp.dot(pick[0], near[0, dist - 1, f], **EXACT) + jnp.dot(pick[1], near[1, dist - 1, f], **EXACT),
        )
        send_in_plane(g, f)

    def first_hop(f):
        for way in range(2):
            hop_copy(0, way, f).wait_recv()
            hop_copy(1, way, f).start()
        if f == 0:
            shared.wait_recv()
            choose_pair(1, 1)
        put_pair(1, 1, f)

    def second_hop(f):
        for way in range(2):
            hop_copy(1, way, f).wait_recv()
            hop[way, f] = jnp.dot(pickr[way], near[way, 1, f], **EXACT).astype(BF16)
            hop_copy(2, way, f).start()
        put_pair(2, 2, f)

    def spread(n, a, count):
        i, q = iota((count // CAP * n, count), 0), iota((count // CAP * n, count), 1)
        return as_mask(i == q + div(q, CAP) * (n - CAP) + a * CAP)

    def third_hop(f):
        for way in range(2):
            hop_copy(2, way, f).wait_recv()
            hop_copy(3, way, f).start()
        put(
            3, f,
            jnp.dot(pick[0, :, 0 : 2 * half], far[0, f, half:], **EXACT)
            + jnp.dot(pick[1, :, 0 : 2 * half], far[1, f, half:], **EXACT),
        )
        send_in_plane(3, f)

    def fourth_hop(h):
        half_peers = peers // 2
        for way in range(2):
            total = jnp.zeros((half_peers * 24, wide), F32)
            for a in range(2):
                hop_copy(3, way, 2 * h + a).wait_recv()
                total = total + jnp.dot(pick[a, 0 : half_peers * 24, 0:half], last[way, 2 * h + a], **EXACT)
            sb[4][h, way * half_peers : (way + 1) * half_peers] = (
                total.reshape(half_peers, 24, wide).astype(BF16)
            )
        send_in_plane(4, h)

    first_hop(0)
    first_hop(1)
    local(w1, w1, wsem.at[1]).wait()
    local(w2, w2, wsem.at[2]).wait()
    expert(0)
    first_hop(2)

    for way in range(2):
        d = 2 if way == 0 else Z - 2
        p3, p4 = up_z(sign[way]), up_z(2 * sign[way])
        q4 = target((2 * half, 1), 0, CAP, 0, p4)
        pickr[way, 0:half, :] = chooser(q4[way * half : (way + 1) * half], d)
        pickr[way, half:, :] = chooser(target((2 * half, 1), 0, CAP, 0, p3), d)

    remote(lrecv, lrecv, msend.at[1], mrecv.at[1], along_x(1)).wait_recv()
    logit = lpart[x] + lrecv[0] + lrecv[1] + lrecv[2]
    row_top = jnp.max(logit, axis=1, keepdims=True)
    term = jnp.exp(logit - row_top)
    row_total = jnp.sum(term, axis=1, keepdims=True)
    col = cols[x]
    lane = iota((share, experts), 1)
    both = []
    for k in range(2):
        chosen = jnp.sum(jnp.where(lane == col[:, k : k + 1].astype(I32), term, 0.0), axis=1, keepdims=True)
        both.append(experts * chosen / row_total * col[:, 4:5])
    wide_lane = iota((share, fac.shape[2]), 1)
    fac[x] = jnp.where(wide_lane == 0, both[0], jnp.where(wide_lane == 1, both[1], 0.0))

    def factor_copy(d):
        return remote(fac.at[x], fac.at[x], msend.at[2], mrecv.at[2], along_x(d))

    for d in range(1, X):
        factor_copy(d).start()

    back_in_plane(0)
    add_up(z, 16, rb[0][...].reshape(peers * 16, rb[0].shape[2]), True)

    def gather_back(d):
        back_copy(d).wait_recv()
        add_up(up_z(d), CAP, zr[d])

    first_hop(3)
    choose_pair(2, 2)
    second_hop(0)
    expert(1)
    second_hop(1)
    back_in_plane(1)
    sort_back(1, (1, Z - 1))
    second_hop(2)
    second_hop(3)
    for a in range(2):
        pick[a, :, 0 : 2 * half] = spread(24, a, 2 * half)
    last_slots = target((1, 2 * half), 1, CAP, 0, up_z(4))
    for k in range(2):
        col = cols[...].reshape(rows, 8)
        p = (col[:, k : k + 1] * CAP + col[:, 2 + k : 3 + k]).astype(I32)
        pick[k, :, 2 * half : 4 * half] = as_mask(p == last_slots)
    third_hop(0)
    expert(2)
    third_hop(1)
    partly(3, 0)
    third_hop(2)
    back_in_plane(2)
    sort_back(2, (2, Z - 2))
    third_hop(3)
    for d in near_z:
        back_copy(d).start()
    partly(3, 1)
    fourth_hop(0)
    partly(3, 2)
    finish(3)
    fourth_hop(1)
    partly(4, 0)
    partly(4, 1)
    back_in_plane(3)
    sort_back(3, (3, Z - 3))
    partly(4, 2)
    finish(4)
    back_in_plane(4)
    sort_back(4, (4,))
    for d in (1, 7, 2, 6, 3, 5):
        gather_back(d)

    block = fac.at[pl.ds(0, X - 1)]
    remote(block, block, msend.at[2], mrecv.at[2], along_x(1)).wait_recv()
    scale = fac[...].reshape(rows, fac.shape[2])
    for step, whole in enumerate((near.at[:, 0], near.at[:, 1], hop, last)):
        remote(whole, whole, hsend.at[step], hrecv.at[0, step, 0], at_z(1)).wait_send()
    shared.wait_send()
    remote(lrecv, lrecv, msend.at[1], mrecv.at[1], along_x(1)).wait_send()
    remote(block, block, msend.at[2], mrecv.at[2], along_x(1)).wait_send()
    for g in range(5):
        sent = xb[g].at[:, pl.ds(0, peers - 1)]
        remote(sent, sent, isend.at[g], irecv.at[g, 0], along_x(1)).wait_send()
        sent = rb[g].at[pl.ds(0, peers - 1)]
        remote(sent, sent, rsend.at[g], rrecv.at[g], along_x(1)).wait_send()
    sent = zs.at[pl.ds(1, Z - 1)]
    remote(sent, sent, zsend.at[0], zrecv.at[1], at_z(1)).wait_send()

    back_copy(4).wait_recv()
    final = [acc[k] + jnp.dot(pick[k, :, 2 * half : 4 * half], zr[4], **EXACT) for k in range(2)]
    out[...] = (scale[:, 0:1] * final[0] + scale[:, 1:2] * final[1]).astype(out.dtype)


def per_device(samples, gate_weight, expert_ids, pad_mask, up_weight, down_weight):
    rows, share = samples.shape
    experts = gate_weight.shape[1]
    depth, hidden = up_weight.shape[1:]
    columns = down_weight.shape[2] // X
    peers = Y * C * X
    nf = 4
    wide = share // nf
    width = (16, 24, 24, 24, 16)
    slots = peers * CAP
    dma = pltpu.SemaphoreType.DMA
    any_space = pl.BlockSpec(memory_space=pl.ANY)
    vmem = pl.BlockSpec(memory_space=pltpu.VMEM)
    scratch = [
        pltpu.VMEM((nf, rows, wide), BF16),
        pltpu.VMEM(gate_weight.shape, BF16),
        pltpu.VMEM((4, nf, X, wide, hidden // 4), BF16),
        pltpu.VMEM((4, hidden, columns), BF16),
        pltpu.VMEM((2, 2, nf, rows, wide), BF16),
        pltpu.VMEM((2, nf, slots * 3 // 2, wide), BF16),
        pltpu.VMEM((2, nf, slots * 3 // 2, wide), BF16),
        pltpu.VMEM((2, nf, slots // 2, wide), BF16),
    ]
    messages = [(nf, peers, n, wide) for n in width[:4]] + [(nf // 2, peers, 24, wide)]
    scratch += [pltpu.VMEM(shape, BF16) for shape in messages * 2]
    scratch += [pltpu.VMEM((X, Y * C, n, columns), BF16) for n in width]
    scratch += [pltpu.VMEM((peers, n, columns), BF16) for n in width]
    scratch += [
        pltpu.VMEM((Z, slots, columns), BF16),
        pltpu.VMEM((Z, slots, columns), BF16),
        pltpu.VMEM((Z, 2, rows), I32),
        pltpu.VMEM((8, rows), F32),
        pltpu.VMEM((2, peers * 24, rows), BF16),
        pltpu.VMEM((2, slots * 3 // 2, rows), BF16),
        pltpu.VMEM((X, rows // X, 8), F32),
        pltpu.VMEM((X, rows // X, experts), F32),
        pltpu.VMEM((X - 1, rows // X, experts), F32),
        pltpu.VMEM((X, rows // X, 128), F32),
        pltpu.VMEM((4, Y * C * 24, hidden // 4), BF16),
        pltpu.VMEM((2, rows, columns), F32),
        pltpu.VMEM((2, 4, Y * C * 24, hidden // 4), F32),
        pltpu.VMEM((Y * C * 16, depth // 4), BF16),
    ]
    scratch += [
        dma((3,)), dma((nf,)), pltpu.SemaphoreType.REGULAR((7,)), dma((4,)), dma((2, 4, nf)), dma((5,)), dma((5, nf)),
        dma((5,)), dma((5,)), dma((1,)), dma((Z,)), dma((3,)), dma((3,)),
    ]
    return pl.pallas_call(
        kernel,
        out_shape=jax.ShapeDtypeStruct((rows, columns), BF16),
        in_specs=[any_space, any_space, vmem, vmem, any_space, any_space],
        out_specs=vmem,
        scratch_shapes=scratch,
        compiler_params=pltpu.CompilerParams(
            collective_id=0, has_side_effects=True, vmem_limit_bytes=67043328
        ),
    )(samples, gate_weight, expert_ids.T, pad_mask,
      up_weight.reshape(X, nf, wide, hidden), down_weight)


def solution(mesh):
    placed = (
        P("expert", "gate"),
        P("gate", None),
        P("expert", None),
        P("expert"),
        P(("expert", "gate"), None, None),
        P(("expert", "gate"), None, None),
    )
    return jax.shard_map(
        per_device, mesh=mesh, in_specs=placed, out_specs=P("expert", "gate"), check_vma=False
    )
```

```python
import jax
import jax.numpy as jnp
from jax import lax
from jax.experimental import pallas as pl
from jax.experimental.pallas import tpu as pltpu
from jax.sharding import PartitionSpec as P

MESH = pl.DeviceIdType.MESH
Y, Z, C, X = 4, 8, 2, 4
CAP = 12
F32, BF16, I32 = jnp.float32, jnp.bfloat16, jnp.int32
EXACT = dict(preferred_element_type=F32)


def iota(shape, dim):
    return lax.broadcasted_iota(I32, shape, dim)


def div(v, n):
    return lax.shift_right_logical(v * (-(-(1 << 17) // n)), 17)


def as_mask(cond):
    return jnp.where(cond, 1.0, 0.0).astype(BF16)


def kernel(
    samples, gate, ids, mask, up, down, out,
    sv, gv, w1, w2, near, hop, far, last,
    sb0, sb1, sb2, sb3, sb4, xb0, xb1, xb2, xb3, xb4,
    ob0, ob1, ob2, ob3, ob4, rb0, rb1, rb2, rb3, rb4,
    zs, zr, posb, rowb, pick, pickr, cols, lpart, lrecv, fac, act, acc, hid, apart, done,
    wsem, ssem, known, hsend, hrecv, isend, irecv, rsend, rrecv, zsend, zrecv, msend, mrecv,
):
    sb, xb = (sb0, sb1, sb2, sb3, sb4), (xb0, xb1, xb2, xb3, xb4)
    ob, rb = (ob0, ob1, ob2, ob3, ob4), (rb0, rb1, rb2, rb3, rb4)
    width = (16, 24, 24, 24, 16)
    ne = lax.axis_index("expert")
    x = lax.axis_index("gate")
    y, z, c = ne // (Z * C), (ne // C) % Z, ne % C
    half = Y * C * X * CAP // 2
    nf = sv.shape[0]
    rows = sv.shape[1]
    wide = sv.shape[2]
    share = rows // X

    def up_z(d):
        return lax.rem(z + d % Z, Z)

    def at_z(d):
        return (y * Z + up_z(d)) * C + c, x

    peers = Y * C * X

    def to_plane(visit):
        order = [(dx, dc) for dx in (2, 1, 3, 0) for dc in (1, 0)]

        def one(i, dx, dc):
            y2, c2, x2 = lax.rem(y + dx + i, Y), lax.rem(c + dc, C), lax.rem(x + dx, X)
            visit(y2, c2, x2, ((y2 * Z + z) * C + c2, x2))

        def some(i, carry):
            for dx, dc in order:
                one(i, dx, dc)
            return carry

        for dx, dc in order[:-1]:
            one(0, dx, dc)
        lax.fori_loop(1, Y, some, 0)

    mine = (y * C + c) * X + x
    source = x * (Y * C) + y * C + c

    def remote(src, dst, ss, rs, dev):
        return pltpu.make_async_remote_copy(
            src_ref=src, dst_ref=dst, send_sem=ss, recv_sem=rs, device_id=dev, device_id_type=MESH
        )

    barrier = pltpu.get_barrier_semaphore()
    z_near = (at_z(1), at_z(-1))
    y_near = tuple(((lax.rem(y + d, Y) * Z + z) * C + c, x) for d in (1, Y - 1))
    x_near = tuple((ne, lax.rem(x + d, X)) for d in (1, X - 1))
    partner = (((y * Z + z) * C + lax.rem(c + 1, C), x),)
    neighbours = z_near + y_near + x_near + partner
    for dev in neighbours:
        pl.semaphore_signal(barrier, inc=1, device_id=dev, device_id_type=MESH)

    def tell(i, devices):
        for dev in devices:
            pl.semaphore_signal(known.at[i], inc=1, device_id=dev, device_id_type=MESH)

    def heard(i, devices):
        pl.semaphore_wait(known.at[i], len(devices))

    def local(src, dst, sem):
        return pltpu.make_async_copy(src, dst, sem)

    fetch_s = [local(samples.at[:, pl.ds(f * wide, wide)], sv.at[f], ssem.at[f]) for f in range(nf)]
    for copy in fetch_s:
        copy.start()
    fetch_g = local(gate, gv, wsem.at[0])
    fetch_g.start()
    nt = w1.shape[0]
    hw, ow = w1.shape[4], w2.shape[2]
    fetch_1 = [
        local(up.at[xs, :, :, pl.ds(j * hw, hw)], w1.at[j, :, xs], wsem.at[1])
        for j in range(nt)
        for xs in range(X)
    ]
    fetch_2 = [
        local(down.at[0, :, pl.ds(j * ow, ow)], w2.at[j], wsem.at[2]) for j in range(nt)
    ]
    for copy in fetch_1 + fetch_2:
        copy.start()

    with jax.named_scope("greet"):
        pl.semaphore_wait(barrier, len(neighbours))

    sign = (1, -1)

    def hop_copy(step, way, f):
        dev = at_z(sign[way])
        sems = hsend.at[step], hrecv.at[way, step, f]
        if step == 0:
            src, dst = sv.at[f], near.at[way, 0, f]
        elif step == 1:
            src, dst = near.at[way, 0, f], near.at[way, 1, f]
        elif step == 2:
            src, dst = hop.at[way, f], far.at[way, f]
        else:
            src, dst = far.at[way, f, pl.ds(0, half)], last.at[way, f]
        return remote(src, dst, *sems, dev)

    for f in range(nf):
        fetch_s[f].wait()
        if f == 0:
            hop_copy(0, 0, 0).start()
            hop_copy(0, 1, 0).start()
            tell(0, x_near)
            tell(1, z_near)

    experts = gate.shape[1]
    earlier = as_mask(iota((rows, rows), 0) < iota((rows, rows), 1))
    named = [as_mask(iota((experts, rows), 0) == ids[k : k + 1, :]) for k in range(2)]
    count = jnp.dot((named[0].astype(F32) + named[1].astype(F32)).astype(BF16), earlier, **EXACT)
    rowb[...] = jnp.zeros_like(rowb)
    for k in range(2):
        rank = jnp.sum(named[k].astype(F32) * count, axis=0, keepdims=True)
        posb[0, k : k + 1, :] = ids[k : k + 1, :] * CAP + rank.astype(I32)
        rowb[k : k + 1, :] = ids[k : k + 1, :].astype(F32)
        rowb[2 + k : 3 + k, :] = rank
    rowb[4:5, :] = mask[...].reshape(1, rows).astype(F32)

    def pos_copy(d):
        return remote(posb.at[0], posb.at[d], msend.at[0], mrecv.at[0], at_z(d))

    heard(1, z_near)
    tell(2, z_near)
    heard(0, x_near)
    tell(3, y_near)
    near_z = (1, Z - 1, 2, Z - 2)
    for d in near_z:
        pos_copy(d).start()
    for f in range(1, nf):
        hop_copy(0, 0, f).start()
        hop_copy(0, 1, f).start()

    same = as_mask(iota((rows, rows), 0) == iota((rows, rows), 1))
    turned = lax.dot_general(same, rowb[...].astype(BF16), (((1,), (1,)), ((), ())), **EXACT)
    cols[...] = turned.reshape(cols.shape)
    heard(3, y_near)
    tell(4, y_near)
    heard(2, z_near)
    tell(5, z_near)

    def target(shape, dim, n, a, plane):
        i = iota(shape, dim)
        if n == CAP:
            block, j = div(i, CAP * C * X), i
            return block * (Z * C * X * CAP - C * X * CAP) + plane * (C * X * CAP) + j
        d = div(i, n)
        s = i - d * n - a * CAP
        block = lax.shift_right_logical(d, 3)
        slot = block * (Z * C * X * CAP) + plane * (C * X * CAP) + (d - block * (C * X)) * CAP + s
        return jnp.where((s >= 0) & (s < CAP), slot, -1)

    def chooser(slots, d):
        p0, p1 = posb[d, 0:1, :], posb[d, 1:2, :]
        return as_mask((slots == p0) | (slots == p1))

    def put(g, f, value):
        sb[g][f] = value.reshape(peers, width[g], wide).astype(BF16)

    def send_in_plane(g, f):
        def one(y2, c2, x2, dev):
            to = (y2 * C + c2) * X + x2
            remote(sb[g].at[f, to], xb[g].at[f, source], isend.at[g], irecv.at[g, f], dev).start()

        to_plane(one)
        xb[g][f, source] = sb[g][f, mine]

    def dispatched(g, f):
        part = xb[g].at[f, pl.ds(0, peers - 1)]
        return remote(part, part, isend.at[g], irecv.at[g, f], along_x(1))

    def along_x(d):
        return ne, lax.rem(x + d, X)

    fetch_g.wait()
    logits = jnp.zeros((rows, experts), F32)
    for f in range(nf):
        logits = logits + jnp.dot(sv[f], gv[f * wide : (f + 1) * wide, :], **EXACT)
    lpart[...] = logits.reshape(lpart.shape)

    def logit_copy(d):
        return remote(lpart.at[lax.rem(x + d, X)], lrecv.at[d - 1], msend.at[1], mrecv.at[1], along_x(d))

    for d in range(1, X):
        logit_copy(d).start()

    heard(4, y_near)
    tell(6, partner)
    heard(5, z_near)
    pick[0, : peers * 16, :] = chooser(target((peers * 16, 1), 0, 16, 0, z), 0)
    for f in range(nf):
        put(0, f, jnp.dot(pick[0, : peers * 16, :], sv[f], **EXACT))
        if f == 0:
            heard(6, partner)
        send_in_plane(0, f)

    m_of = [Y * C * n for n in width]

    def features(g, f):
        part = [xb[g][f, xs * Y * C : (xs + 1) * Y * C].reshape(m_of[g], wide) for xs in range(X)]
        return jnp.concatenate(part, axis=1)

    def layer_1(g, f, j):
        part = features(g, f) if g < 4 else apart[...]
        return jnp.dot(part, w1[j, f].reshape(X * wide, hw), **EXACT)

    def partly(g, f):
        m = m_of[g]
        if g < 4:
            dispatched(g, f).wait_recv()
        else:
            h, a = f // 2, f % 2
            if a == 0:
                dispatched(g, h).wait_recv()
            i, r = iota((m, Y * C * 24), 1), iota((m, Y * C * 24), 0)
            p = lax.shift_right_logical(r, 4)
            keep = (i == p * 24 + (r - p * 16) + a * CAP) & (r - p * 16 < CAP)
            both = [xb[g][h, xs * Y * C : (xs + 1) * Y * C].reshape(Y * C * 24, wide) for xs in range(X)]
            for xs in range(X):
                part = jnp.dot(as_mask(keep), both[xs], **EXACT)
                apart[:, xs * wide : (xs + 1) * wide] = part.astype(BF16)

        def one(j, carry):
            if f == 0:
                hid[g - 3, j, 0:m, :] = layer_1(g, f, j)
            else:
                hid[g - 3, j, 0:m, :] += layer_1(g, f, j)
            return carry

        lax.fori_loop(0, nt, one, 0)

    def outward(g):
        n, m = width[g], m_of[g]
        for dx in (2, 1, 3, 0):
            x2 = lax.rem(x + dx, X)
            whole = jnp.concatenate([act[i, 0:m, :] for i in range(nt)], axis=1)
            total = jnp.dot(whole, w2[x2], **EXACT)
            ob[g][x2] = total.reshape(Y * C, n, ow).astype(BF16)
            for dy in (2, 1, 3, 0):
                for dc in range(C):
                    y2, c2 = lax.rem(y + dy, Y), lax.rem(c + dc, C)
                    if dx + dy + dc:
                        dev = (y2 * Z + z) * C + c2, x2
                        remote(ob[g].at[x2, y2 * C + c2], rb[g].at[mine], rsend.at[g], rrecv.at[g], dev).start()
        rb[g][mine] = ob[g][x, y * C + c]

    def expert(g):
        m = m_of[g]
        for f in range(nf):
            dispatched(g, f).wait_recv()

        def first(j, carry):
            total = layer_1(g, 0, j)
            for f in range(1, nf):
                total = total + layer_1(g, f, j)
            act[j, 0:m, :] = jnp.maximum(total, 0.0).astype(BF16)
            return carry

        lax.fori_loop(0, nt, first, 0)
        outward(g)

    def finish(g):
        m = m_of[g]
        partly(g, nf - 1)

        def first(j, carry):
            act[j, 0:m, :] = jnp.maximum(hid[g - 3, j, 0:m, :], 0.0).astype(BF16)
            return carry

        lax.fori_loop(0, nt, first, 0)
        outward(g)

    def back_in_plane(g):
        block = rb[g].at[pl.ds(0, peers - 1)]
        remote(block, block, rsend.at[g], rrecv.at[g], along_x(1)).wait_recv()

    def back_copy(d):
        return remote(zs.at[d], zr.at[d], zsend.at[0], zrecv.at[d], at_z(-d))

    def sort_back(g, sources):
        n = width[g]
        q, i = iota((2 * half, peers * n), 0), iota((2 * half, peers * n), 1)
        base = q + div(q, CAP) * (n - CAP)
        got = rb[g][...].reshape(peers * n, rb[g].shape[2])
        for a, d in enumerate(sources):
            zs[d] = jnp.dot(as_mask(i == base + a * CAP), got, **EXACT).astype(BF16)
            if g > 2:
                back_copy(d).start()

    def add_up(plane, n, values, fresh=False):
        slots = target((1, values.shape[0]), 1, n, 0, plane)
        for k in range(2):
            col = cols[...].reshape(rows, 8)
            p = (col[:, k : k + 1] * CAP + col[:, 2 + k : 3 + k]).astype(I32)
            term = jnp.dot(as_mask(p == slots), values, **EXACT)
            if fresh:
                acc[k] = term
            else:
                acc[k] += term

    shared = posb.at[pl.ds(0, len(near_z))]
    shared = remote(shared, shared, msend.at[0], mrecv.at[0], along_x(1))

    def choose_pair(g, dist):
        n = width[g]
        for a, d in enumerate((dist, Z - dist)):
            pick[a] = chooser(target((peers * n, 1), 0, n, a, z), d)

    def put_pair(g, dist, f):
        put(
            g, f,
            jnp.dot(pick[0], near[0, dist - 1, f], **EXACT) + jnp.dot(pick[1], near[1, dist - 1, f], **EXACT),
        )
        send_in_plane(g, f)

    def first_hop(f):
        for way in range(2):
            hop_copy(0, way, f).wait_recv()
            hop_copy(1, way, f).start()
        if f == 0:
            shared.wait_recv()
            choose_pair(1, 1)
        put_pair(1, 1, f)

    def second_hop(f):
        for way in range(2):
            hop_copy(1, way, f).wait_recv()
            hop[way, f] = jnp.dot(pickr[way], near[way, 1, f], **EXACT).astype(BF16)
            hop_copy(2, way, f).start()
        put_pair(2, 2, f)

    def spread(n, a, count):
        i, q = iota((count // CAP * n, count), 0), iota((count // CAP * n, count), 1)
        return as_mask(i == q + div(q, CAP) * (n - CAP) + a * CAP)

    def third_hop(f):
        for way in range(2):
            hop_copy(2, way, f).wait_recv()
            hop_copy(3, way, f).start()
        put(
            3, f,
            jnp.dot(pick[0, :, 0 : 2 * half], far[0, f, half:], **EXACT)
            + jnp.dot(pick[1, :, 0 : 2 * half], far[1, f, half:], **EXACT),
        )
        send_in_plane(3, f)

    def fourth_hop(h):
        half_peers = peers // 2
        for way in range(2):
            total = jnp.zeros((half_peers * 24, wide), F32)
            for a in range(2):
                hop_copy(3, way, 2 * h + a).wait_recv()
                total = total + jnp.dot(pick[a, 0 : half_peers * 24, 0:half], last[way, 2 * h + a], **EXACT)
            sb[4][h, way * half_peers : (way + 1) * half_peers] = (
                total.reshape(half_peers, 24, wide).astype(BF16)
            )
        send_in_plane(4, h)

    first_hop(0)
    first_hop(1)
    local(w1, w1, wsem.at[1]).wait()
    local(w2, w2, wsem.at[2]).wait()
    expert(0)
    first_hop(2)

    for way in range(2):
        d = 2 if way == 0 else Z - 2
        p3, p4 = up_z(sign[way]), up_z(2 * sign[way])
        q4 = target((2 * half, 1), 0, CAP, 0, p4)
        pickr[way, 0:half, :] = chooser(q4[way * half : (way + 1) * half], d)
        pickr[way, half:, :] = chooser(target((2 * half, 1), 0, CAP, 0, p3), d)

    remote(lrecv, lrecv, msend.at[1], mrecv.at[1], along_x(1)).wait_recv()
    logit = lpart[x] + lrecv[0] + lrecv[1] + lrecv[2]
    row_top = jnp.max(logit, axis=1, keepdims=True)
    term = jnp.exp(logit - row_top)
    row_total = jnp.sum(term, axis=1, keepdims=True)
    col = cols[x]
    lane = iota((share, experts), 1)
    both = []
    for k in range(2):
        chosen = jnp.sum(jnp.where(lane == col[:, k : k + 1].astype(I32), term, 0.0), axis=1, keepdims=True)
        both.append(experts * chosen / row_total * col[:, 4:5])
    wide_lane = iota((share, fac.shape[2]), 1)
    fac[x] = jnp.where(wide_lane == 0, both[0], jnp.where(wide_lane == 1, both[1], 0.0))

    def factor_copy(d):
        return remote(fac.at[x], fac.at[x], msend.at[2], mrecv.at[2], along_x(d))

    for d in range(1, X):
        factor_copy(d).start()

    back_in_plane(0)
    add_up(z, 16, rb[0][...].reshape(peers * 16, rb[0].shape[2]), True)

    def gather_back(d):
        back_copy(d).wait_recv()
        add_up(up_z(d), CAP, zr[d])

    first_hop(3)
    choose_pair(2, 2)
    second_hop(0)
    expert(1)
    second_hop(1)
    back_in_plane(1)
    sort_back(1, (1, Z - 1))
    second_hop(2)
    second_hop(3)
    for a in range(2):
        pick[a, :, 0 : 2 * half] = spread(24, a, 2 * half)
    last_slots = target((1, 2 * half), 1, CAP, 0, up_z(4))
    for k in range(2):
        col = cols[...].reshape(rows, 8)
        p = (col[:, k : k + 1] * CAP + col[:, 2 + k : 3 + k]).astype(I32)
        pick[k, :, 2 * half : 4 * half] = as_mask(p == last_slots)
    third_hop(0)
    expert(2)
    third_hop(1)
    partly(3, 0)
    third_hop(2)
    back_in_plane(2)
    sort_back(2, (2, Z - 2))
    third_hop(3)
    for d in near_z:
        back_copy(d).start()
    partly(3, 1)
    fourth_hop(0)
    partly(3, 2)
    finish(3)
    fourth_hop(1)
    partly(4, 0)
    partly(4, 1)
    back_in_plane(3)
    sort_back(3, (3, Z - 3))
    partly(4, 2)
    finish(4)
    back_in_plane(4)
    sort_back(4, (4,))
    for d in (1, 7, 2, 6, 3, 5):
        gather_back(d)

    block = fac.at[pl.ds(0, X - 1)]
    remote(block, block, msend.at[2], mrecv.at[2], along_x(1)).wait_recv()
    scale = fac[...].reshape(rows, fac.shape[2])
    for step, whole in enumerate((near.at[:, 0], near.at[:, 1], hop, last)):
        remote(whole, whole, hsend.at[step], hrecv.at[0, step, 0], at_z(1)).wait_send()
    shared.wait_send()
    remote(lrecv, lrecv, msend.at[1], mrecv.at[1], along_x(1)).wait_send()
    remote(block, block, msend.at[2], mrecv.at[2], along_x(1)).wait_send()
    for g in range(5):
        sent = xb[g].at[:, pl.ds(0, peers - 1)]
        remote(sent, sent, isend.at[g], irecv.at[g, 0], along_x(1)).wait_send()
        sent = rb[g].at[pl.ds(0, peers - 1)]
        remote(sent, sent, rsend.at[g], rrecv.at[g], along_x(1)).wait_send()
    sent = zs.at[pl.ds(1, Z - 1)]
    remote(sent, sent, zsend.at[0], zrecv.at[1], at_z(1)).wait_send()

    back_copy(4).wait_recv()
    leave = []
    for h in range(2):
        part = slice(h * rows // 2, (h + 1) * rows // 2)
        final = [acc[k, part] + jnp.dot(pick[k, part, 2 * half : 4 * half], zr[4], **EXACT) for k in range(2)]
        done[part] = (scale[part, 0:1] * final[0] + scale[part, 1:2] * final[1]).astype(out.dtype)
        leave.append(local(done.at[part], out.at[part], ssem.at[h]))
        leave[h].start()
    for copy in leave:
        copy.wait()


def per_device(samples, gate_weight, expert_ids, pad_mask, up_weight, down_weight):
    rows, share = samples.shape
    experts = gate_weight.shape[1]
    depth, hidden = up_weight.shape[1:]
    columns = down_weight.shape[2] // X
    peers = Y * C * X
    nf = 4
    wide = share // nf
    width = (16, 24, 24, 24, 16)
    slots = peers * CAP
    dma = pltpu.SemaphoreType.DMA
    any_space = pl.BlockSpec(memory_space=pl.ANY)
    vmem = pl.BlockSpec(memory_space=pltpu.VMEM)
    scratch = [
        pltpu.VMEM((nf, rows, wide), BF16),
        pltpu.VMEM(gate_weight.shape, BF16),
        pltpu.VMEM((4, nf, X, wide, hidden // 4), BF16),
        pltpu.VMEM((4, hidden, columns), BF16),
        pltpu.VMEM((2, 2, nf, rows, wide), BF16),
        pltpu.VMEM((2, nf, slots * 3 // 2, wide), BF16),
        pltpu.VMEM((2, nf, slots * 3 // 2, wide), BF16),
        pltpu.VMEM((2, nf, slots // 2, wide), BF16),
    ]
    messages = [(nf, peers, n, wide) for n in width[:4]] + [(nf // 2, peers, 24, wide)]
    scratch += [pltpu.VMEM(shape, BF16) for shape in messages * 2]
    scratch += [pltpu.VMEM((X, Y * C, n, columns), BF16) for n in width]
    scratch += [pltpu.VMEM((peers, n, columns), BF16) for n in width]
    scratch += [
        pltpu.VMEM((Z, slots, columns), BF16),
        pltpu.VMEM((Z, slots, columns), BF16),
        pltpu.VMEM((Z, 2, rows), I32),
        pltpu.VMEM((8, rows), F32),
        pltpu.VMEM((2, peers * 24, rows), BF16),
        pltpu.VMEM((2, slots * 3 // 2, rows), BF16),
        pltpu.VMEM((X, rows // X, 8), F32),
        pltpu.VMEM((X, rows // X, experts), F32),
        pltpu.VMEM((X - 1, rows // X, experts), F32),
        pltpu.VMEM((X, rows // X, 128), F32),
        pltpu.VMEM((4, Y * C * 24, hidden // 4), BF16),
        pltpu.VMEM((2, rows, columns), F32),
        pltpu.VMEM((2, 4, Y * C * 24, hidden // 4), F32),
        pltpu.VMEM((Y * C * 16, depth // 4), BF16),
        pltpu.VMEM((rows, columns), BF16),
    ]
    scratch += [
        dma((3,)), dma((nf,)), pltpu.SemaphoreType.REGULAR((7,)), dma((4,)), dma((2, 4, nf)), dma((5,)), dma((5, nf)),
        dma((5,)), dma((5,)), dma((1,)), dma((Z,)), dma((3,)), dma((3,)),
    ]
    return pl.pallas_call(
        kernel,
        out_shape=jax.ShapeDtypeStruct((rows, columns), BF16),
        in_specs=[any_space, any_space, vmem, vmem, any_space, any_space],
        out_specs=any_space,
        scratch_shapes=scratch,
        compiler_params=pltpu.CompilerParams(
            collective_id=0, has_side_effects=True, vmem_limit_bytes=67043328
        ),
    )(samples, gate_weight, expert_ids.T, pad_mask,
      up_weight.reshape(X, nf, wide, hidden), down_weight)


def solution(mesh):
    placed = (
        P("expert", "gate"),
        P("gate", None),
        P("expert", None),
        P("expert"),
        P(("expert", "gate"), None, None),
        P(("expert", "gate"), None, None),
    )
    return jax.shard_map(
        per_device, mesh=mesh, in_specs=placed, out_specs=P("expert", "gate"), check_vma=False
    )
```

```python
import jax
import jax.numpy as jnp
from jax import lax
from jax.experimental import pallas as pl
from jax.experimental.pallas import tpu as pltpu
from jax.sharding import PartitionSpec as P

MESH = pl.DeviceIdType.MESH
Y, Z, C, X = 4, 8, 2, 4
CAP = 12
F32, BF16, I32 = jnp.float32, jnp.bfloat16, jnp.int32
EXACT = dict(preferred_element_type=F32)


def iota(shape, dim):
    return lax.broadcasted_iota(I32, shape, dim)


def div(v, n):
    return lax.shift_right_logical(v * (-(-(1 << 17) // n)), 17)


def as_mask(cond):
    return jnp.where(cond, 1.0, 0.0).astype(BF16)


def kernel(
    samples, gate, ids, mask, up, down, out,
    sv, gv, w1, w2, near, hop, far, last,
    sb0, sb1, sb2, sb3, sb4, xb0, xb1, xb2, xb3, xb4,
    ob0, ob1, ob2, ob3, ob4, rb0, rb1, rb2, rb3, rb4,
    zs, zr, posb, rowb, pick, pickr, cols, lpart, lrecv, fac, act, acc, hid, apart,
    wsem, ssem, known, hsend, hrecv, isend, irecv, rsend, rrecv, zsend, zrecv, msend, mrecv,
):
    sb, xb = (sb0, sb1, sb2, sb3, sb4), (xb0, xb1, xb2, xb3, xb4)
    ob, rb = (ob0, ob1, ob2, ob3, ob4), (rb0, rb1, rb2, rb3, rb4)
    width = (16, 24, 24, 24, 16)
    ne = lax.axis_index("expert")
    x = lax.axis_index("gate")
    y, z, c = ne // (Z * C), (ne // C) % Z, ne % C
    half = Y * C * X * CAP // 2
    nf = sv.shape[0]
    rows = sv.shape[1]
    wide = sv.shape[2]
    share = rows // X

    def up_z(d):
        return lax.rem(z + d % Z, Z)

    def at_z(d):
        return (y * Z + up_z(d)) * C + c, x

    peers = Y * C * X

    def to_plane(visit):
        order = [(dx, dc) for dx in (2, 1, 3, 0) for dc in (1, 0)]

        def one(i, dx, dc):
            y2, c2, x2 = lax.rem(y + dx + i, Y), lax.rem(c + dc, C), lax.rem(x + dx, X)
            visit(y2, c2, x2, ((y2 * Z + z) * C + c2, x2))

        def some(i, carry):
            for dx, dc in order:
                one(i, dx, dc)
            return carry

        for dx, dc in order[:-1]:
            one(0, dx, dc)
        lax.fori_loop(1, Y, some, 0)

    mine = (y * C + c) * X + x
    source = x * (Y * C) + y * C + c

    def remote(src, dst, ss, rs, dev):
        return pltpu.make_async_remote_copy(
            src_ref=src, dst_ref=dst, send_sem=ss, recv_sem=rs, device_id=dev, device_id_type=MESH
        )

    barrier = pltpu.get_barrier_semaphore()
    z_near = (at_z(1), at_z(-1))
    y_near = tuple(((lax.rem(y + d, Y) * Z + z) * C + c, x) for d in (1, Y - 1))
    x_near = tuple((ne, lax.rem(x + d, X)) for d in (1, X - 1))
    partner = (((y * Z + z) * C + lax.rem(c + 1, C), x),)
    neighbours = z_near + y_near + x_near + partner
    for dev in neighbours:
        pl.semaphore_signal(barrier, inc=1, device_id=dev, device_id_type=MESH)

    def tell(i, devices):
        for dev in devices:
            pl.semaphore_signal(known.at[i], inc=1, device_id=dev, device_id_type=MESH)

    def heard(i, devices):
        pl.semaphore_wait(known.at[i], len(devices))

    def local(src, dst, sem):
        return pltpu.make_async_copy(src, dst, sem)

    fetch_s = [local(samples.at[:, pl.ds(f * wide, wide)], sv.at[f], ssem.at[f]) for f in range(nf)]
    for copy in fetch_s:
        copy.start()
    fetch_g = local(gate, gv, wsem.at[0])
    fetch_g.start()
    nt = w1.shape[0]
    hw, ow = w1.shape[4], w2.shape[2]
    fetch_1 = [
        local(up.at[xs, :, :, pl.ds(j * hw, hw)], w1.at[j, :, xs], wsem.at[1])
        for j in range(nt)
        for xs in range(X)
    ]
    fetch_2 = [
        local(down.at[0, :, pl.ds(j * ow, ow)], w2.at[j], wsem.at[2]) for j in range(nt)
    ]
    for copy in fetch_1 + fetch_2:
        copy.start()

    with jax.named_scope("greet"):
        pl.semaphore_wait(barrier, len(neighbours))

    sign = (1, -1)

    def hop_copy(step, way, f):
        dev = at_z(sign[way])
        sems = hsend.at[step], hrecv.at[way, step, f]
        if step == 0:
            src, dst = sv.at[f], near.at[way, 0, f]
        elif step == 1:
            src, dst = near.at[way, 0, f], near.at[way, 1, f]
        elif step == 2:
            src, dst = hop.at[way, f], far.at[way, f]
        else:
            src, dst = far.at[way, f, pl.ds(0, half)], last.at[way, f]
        return remote(src, dst, *sems, dev)

    for f in range(nf):
        fetch_s[f].wait()
        if f == 0:
            hop_copy(0, 0, 0).start()
            hop_copy(0, 1, 0).start()
            tell(0, x_near)
            tell(1, z_near)

    experts = gate.shape[1]
    earlier = as_mask(iota((rows, rows), 0) < iota((rows, rows), 1))
    named = [as_mask(iota((experts, rows), 0) == ids[k : k + 1, :]) for k in range(2)]
    count = jnp.dot((named[0].astype(F32) + named[1].astype(F32)).astype(BF16), earlier, **EXACT)
    rowb[...] = jnp.zeros_like(rowb)
    for k in range(2):
        rank = jnp.sum(named[k].astype(F32) * count, axis=0, keepdims=True)
        posb[0, k : k + 1, :] = ids[k : k + 1, :] * CAP + rank.astype(I32)
        rowb[k : k + 1, :] = ids[k : k + 1, :].astype(F32)
        rowb[2 + k : 3 + k, :] = rank
    rowb[4:5, :] = mask[...].reshape(1, rows).astype(F32)

    def pos_copy(d):
        return remote(posb.at[0], posb.at[d], msend.at[0], mrecv.at[0], at_z(d))

    heard(1, z_near)
    tell(2, z_near)
    heard(0, x_near)
    tell(3, y_near)
    near_z = (1, Z - 1, 2, Z - 2)
    for d in near_z:
        pos_copy(d).start()
    for f in range(1, nf):
        hop_copy(0, 0, f).start()
        hop_copy(0, 1, f).start()

    same = as_mask(iota((rows, rows), 0) == iota((rows, rows), 1))
    turned = lax.dot_general(same, rowb[...].astype(BF16), (((1,), (1,)), ((), ())), **EXACT)
    cols[...] = turned.reshape(cols.shape)
    heard(3, y_near)
    tell(4, y_near)
    heard(2, z_near)
    tell(5, z_near)

    def target(shape, dim, n, a, plane):
        i = iota(shape, dim)
        if n == CAP:
            block, j = div(i, CAP * C * X), i
            return block * (Z * C * X * CAP - C * X * CAP) + plane * (C * X * CAP) + j
        d = div(i, n)
        s = i - d * n - a * CAP
        block = lax.shift_right_logical(d, 3)
        slot = block * (Z * C * X * CAP) + plane * (C * X * CAP) + (d - block * (C * X)) * CAP + s
        return jnp.where((s >= 0) & (s < CAP), slot, -1)

    def chooser(slots, d):
        p0, p1 = posb[d, 0:1, :], posb[d, 1:2, :]
        return as_mask((slots == p0) | (slots == p1))

    def put(g, f, value):
        sb[g][f] = value.reshape(peers, width[g], wide).astype(BF16)

    def send_in_plane(g, f):
        def one(y2, c2, x2, dev):
            to = (y2 * C + c2) * X + x2
            remote(sb[g].at[f, to], xb[g].at[f, source], isend.at[g], irecv.at[g, f], dev).start()

        to_plane(one)
        xb[g][f, source] = sb[g][f, mine]

    def dispatched(g, f):
        part = xb[g].at[f, pl.ds(0, peers - 1)]
        return remote(part, part, isend.at[g], irecv.at[g, f], along_x(1))

    def along_x(d):
        return ne, lax.rem(x + d, X)

    fetch_g.wait()
    logits = jnp.zeros((rows, experts), F32)
    for f in range(nf):
        logits = logits + jnp.dot(sv[f], gv[f * wide : (f + 1) * wide, :], **EXACT)
    lpart[...] = logits.reshape(lpart.shape)

    def logit_copy(d):
        return remote(lpart.at[lax.rem(x + d, X)], lrecv.at[d - 1], msend.at[1], mrecv.at[1], along_x(d))

    for d in range(1, X):
        logit_copy(d).start()

    heard(4, y_near)
    tell(6, partner)
    heard(5, z_near)
    pick[0, : peers * 16, :] = chooser(target((peers * 16, 1), 0, 16, 0, z), 0)
    for f in range(nf):
        put(0, f, jnp.dot(pick[0, : peers * 16, :], sv[f], **EXACT))
        if f == 0:
            heard(6, partner)
        send_in_plane(0, f)

    m_of = [Y * C * n for n in width]

    def features(g, f):
        part = [xb[g][f, xs * Y * C : (xs + 1) * Y * C].reshape(m_of[g], wide) for xs in range(X)]
        return jnp.concatenate(part, axis=1)

    def layer_1(g, f, j):
        part = features(g, f) if g < 4 else apart[...]
        return jnp.dot(part, w1[j, f].reshape(X * wide, hw), **EXACT)

    def partly(g, f):
        m = m_of[g]
        if g < 4:
            dispatched(g, f).wait_recv()
        else:
            h, a = f // 2, f % 2
            if a == 0:
                dispatched(g, h).wait_recv()
            i, r = iota((m, Y * C * 24), 1), iota((m, Y * C * 24), 0)
            p = lax.shift_right_logical(r, 4)
            keep = (i == p * 24 + (r - p * 16) + a * CAP) & (r - p * 16 < CAP)
            both = [xb[g][h, xs * Y * C : (xs + 1) * Y * C].reshape(Y * C * 24, wide) for xs in range(X)]
            for xs in range(X):
                part = jnp.dot(as_mask(keep), both[xs], **EXACT)
                apart[:, xs * wide : (xs + 1) * wide] = part.astype(BF16)

        def one(j, carry):
            if f == 0:
                hid[g - 3, j, 0:m, :] = layer_1(g, f, j)
            else:
                hid[g - 3, j, 0:m, :] += layer_1(g, f, j)
            return carry

        lax.fori_loop(0, nt, one, 0)

    def outward(g):
        n, m = width[g], m_of[g]
        for dx in (2, 1, 3, 0):
            x2 = lax.rem(x + dx, X)
            whole = jnp.concatenate([act[i, 0:m, :] for i in range(nt)], axis=1)
            total = jnp.dot(whole, w2[x2], **EXACT)
            ob[g][x2] = total.reshape(Y * C, n, ow).astype(BF16)
            for dy in (2, 1, 3, 0):
                for dc in range(C):
                    y2, c2 = lax.rem(y + dy, Y), lax.rem(c + dc, C)
                    if dx + dy + dc:
                        dev = (y2 * Z + z) * C + c2, x2
                        remote(ob[g].at[x2, y2 * C + c2], rb[g].at[mine], rsend.at[g], rrecv.at[g], dev).start()
        rb[g][mine] = ob[g][x, y * C + c]

    def expert(g):
        m = m_of[g]
        for f in range(nf):
            dispatched(g, f).wait_recv()

        def first(j, carry):
            total = layer_1(g, 0, j)
            for f in range(1, nf):
                total = total + layer_1(g, f, j)
            act[j, 0:m, :] = jnp.maximum(total, 0.0).astype(BF16)
            return carry

        lax.fori_loop(0, nt, first, 0)
        outward(g)

    def finish(g):
        m = m_of[g]
        partly(g, nf - 1)

        def first(j, carry):
            act[j, 0:m, :] = jnp.maximum(hid[g - 3, j, 0:m, :], 0.0).astype(BF16)
            return carry

        lax.fori_loop(0, nt, first, 0)
        outward(g)

    def back_in_plane(g):
        block = rb[g].at[pl.ds(0, peers - 1)]
        remote(block, block, rsend.at[g], rrecv.at[g], along_x(1)).wait_recv()

    def back_copy(d):
        return remote(zs.at[d], zr.at[d], zsend.at[0], zrecv.at[d], at_z(-d))

    def sort_back(g, sources):
        n = width[g]
        q, i = iota((2 * half, peers * n), 0), iota((2 * half, peers * n), 1)
        base = q + div(q, CAP) * (n - CAP)
        got = rb[g][...].reshape(peers * n, rb[g].shape[2])
        for a, d in enumerate(sources):
            zs[d] = jnp.dot(as_mask(i == base + a * CAP), got, **EXACT).astype(BF16)
            if g > 2:
                back_copy(d).start()

    def add_up(plane, n, values, fresh=False):
        slots = target((1, values.shape[0]), 1, n, 0, plane)
        for k in range(2):
            col = cols[...].reshape(rows, 8)
            p = (col[:, k : k + 1] * CAP + col[:, 2 + k : 3 + k]).astype(I32)
            term = jnp.dot(as_mask(p == slots), values, **EXACT)
            if fresh:
                acc[k] = term
            else:
                acc[k] += term

    shared = posb.at[pl.ds(0, len(near_z))]
    shared = remote(shared, shared, msend.at[0], mrecv.at[0], along_x(1))

    def choose_pair(g, dist):
        n = width[g]
        for a, d in enumerate((dist, Z - dist)):
            pick[a] = chooser(target((peers * n, 1), 0, n, a, z), d)

    def put_pair(g, dist, f):
        put(
            g, f,
            jnp.dot(pick[0], near[0, dist - 1, f], **EXACT) + jnp.dot(pick[1], near[1, dist - 1, f], **EXACT),
        )
        send_in_plane(g, f)

    def first_hop(f):
        for way in range(2):
            hop_copy(0, way, f).wait_recv()
            hop_copy(1, way, f).start()
        if f == 0:
            shared.wait_recv()
            choose_pair(1, 1)
        put_pair(1, 1, f)

    def second_hop(f):
        for way in range(2):
            hop_copy(1, way, f).wait_recv()
            hop[way, f] = jnp.dot(pickr[way], near[way, 1, f], **EXACT).astype(BF16)
            hop_copy(2, way, f).start()
        put_pair(2, 2, f)

    def spread(n, a, count):
        i, q = iota((count // CAP * n, count), 0), iota((count // CAP * n, count), 1)
        return as_mask(i == q + div(q, CAP) * (n - CAP) + a * CAP)

    def third_hop(f):
        for way in range(2):
            hop_copy(2, way, f).wait_recv()
            hop_copy(3, way, f).start()
        put(
            3, f,
            jnp.dot(pick[0, :, 0 : 2 * half], far[0, f, half:], **EXACT)
            + jnp.dot(pick[1, :, 0 : 2 * half], far[1, f, half:], **EXACT),
        )
        send_in_plane(3, f)

    def fourth_hop(h):
        half_peers = peers // 2
        for way in range(2):
            total = jnp.zeros((half_peers * 24, wide), F32)
            for a in range(2):
                hop_copy(3, way, 2 * h + a).wait_recv()
                total = total + jnp.dot(pick[a, 0 : half_peers * 24, 0:half], last[way, 2 * h + a], **EXACT)
            sb[4][h, way * half_peers : (way + 1) * half_peers] = (
                total.reshape(half_peers, 24, wide).astype(BF16)
            )
        send_in_plane(4, h)

    first_hop(0)
    first_hop(1)
    local(w1, w1, wsem.at[1]).wait()
    local(w2, w2, wsem.at[2]).wait()
    expert(0)
    first_hop(2)

    for way in range(2):
        d = 2 if way == 0 else Z - 2
        p3, p4 = up_z(sign[way]), up_z(2 * sign[way])
        q4 = target((2 * half, 1), 0, CAP, 0, p4)
        pickr[way, 0:half, :] = chooser(q4[way * half : (way + 1) * half], d)
        pickr[way, half:, :] = chooser(target((2 * half, 1), 0, CAP, 0, p3), d)

    remote(lrecv, lrecv, msend.at[1], mrecv.at[1], along_x(1)).wait_recv()
    logit = lpart[x] + lrecv[0] + lrecv[1] + lrecv[2]
    row_top = jnp.max(logit, axis=1, keepdims=True)
    term = jnp.exp(logit - row_top)
    row_total = jnp.sum(term, axis=1, keepdims=True)
    col = cols[x]
    lane = iota((share, experts), 1)
    both = []
    for k in range(2):
        chosen = jnp.sum(jnp.where(lane == col[:, k : k + 1].astype(I32), term, 0.0), axis=1, keepdims=True)
        both.append(experts * chosen / row_total * col[:, 4:5])
    wide_lane = iota((share, fac.shape[2]), 1)
    fac[x] = jnp.where(wide_lane == 0, both[0], jnp.where(wide_lane == 1, both[1], 0.0))

    def factor_copy(d):
        return remote(fac.at[x], fac.at[x], msend.at[2], mrecv.at[2], along_x(d))

    for d in range(1, X):
        factor_copy(d).start()

    back_in_plane(0)
    add_up(z, 16, rb[0][...].reshape(peers * 16, rb[0].shape[2]), True)

    def gather_back(d):
        back_copy(d).wait_recv()
        add_up(up_z(d), CAP, zr[d])

    first_hop(3)
    choose_pair(2, 2)
    second_hop(0)
    expert(1)
    second_hop(1)
    back_in_plane(1)
    sort_back(1, (1, Z - 1))
    second_hop(2)
    second_hop(3)
    for a in range(2):
        pick[a, :, 0 : 2 * half] = spread(24, a, 2 * half)
    last_slots = target((1, 2 * half), 1, CAP, 0, up_z(4))
    for k in range(2):
        col = cols[...].reshape(rows, 8)
        p = (col[:, k : k + 1] * CAP + col[:, 2 + k : 3 + k]).astype(I32)
        pick[k, :, 2 * half : 4 * half] = as_mask(p == last_slots)
    third_hop(0)
    third_hop(1)
    expert(2)
    partly(3, 0)
    third_hop(2)
    back_in_plane(2)
    sort_back(2, (2, Z - 2))
    third_hop(3)
    for d in near_z:
        back_copy(d).start()
    partly(3, 1)
    fourth_hop(0)
    partly(3, 2)
    finish(3)
    fourth_hop(1)
    partly(4, 0)
    partly(4, 1)
    back_in_plane(3)
    sort_back(3, (3, Z - 3))
    partly(4, 2)
    finish(4)
    back_in_plane(4)
    sort_back(4, (4,))
    for d in (1, 7, 2, 6, 3, 5):
        gather_back(d)

    block = fac.at[pl.ds(0, X - 1)]
    remote(block, block, msend.at[2], mrecv.at[2], along_x(1)).wait_recv()
    scale = fac[...].reshape(rows, fac.shape[2])
    for step, whole in enumerate((near.at[:, 0], near.at[:, 1], hop, last)):
        remote(whole, whole, hsend.at[step], hrecv.at[0, step, 0], at_z(1)).wait_send()
    shared.wait_send()
    remote(lrecv, lrecv, msend.at[1], mrecv.at[1], along_x(1)).wait_send()
    remote(block, block, msend.at[2], mrecv.at[2], along_x(1)).wait_send()
    for g in range(5):
        sent = xb[g].at[:, pl.ds(0, peers - 1)]
        remote(sent, sent, isend.at[g], irecv.at[g, 0], along_x(1)).wait_send()
        sent = rb[g].at[pl.ds(0, peers - 1)]
        remote(sent, sent, rsend.at[g], rrecv.at[g], along_x(1)).wait_send()
    sent = zs.at[pl.ds(1, Z - 1)]
    remote(sent, sent, zsend.at[0], zrecv.at[1], at_z(1)).wait_send()

    back_copy(4).wait_recv()
    final = [acc[k] + jnp.dot(pick[k, :, 2 * half : 4 * half], zr[4], **EXACT) for k in range(2)]
    out[...] = (scale[:, 0:1] * final[0] + scale[:, 1:2] * final[1]).astype(out.dtype)


def per_device(samples, gate_weight, expert_ids, pad_mask, up_weight, down_weight):
    rows, share = samples.shape
    experts = gate_weight.shape[1]
    depth, hidden = up_weight.shape[1:]
    columns = down_weight.shape[2] // X
    peers = Y * C * X
    nf = 4
    wide = share // nf
    width = (16, 24, 24, 24, 16)
    slots = peers * CAP
    dma = pltpu.SemaphoreType.DMA
    any_space = pl.BlockSpec(memory_space=pl.ANY)
    vmem = pl.BlockSpec(memory_space=pltpu.VMEM)
    scratch = [
        pltpu.VMEM((nf, rows, wide), BF16),
        pltpu.VMEM(gate_weight.shape, BF16),
        pltpu.VMEM((4, nf, X, wide, hidden // 4), BF16),
        pltpu.VMEM((4, hidden, columns), BF16),
        pltpu.VMEM((2, 2, nf, rows, wide), BF16),
        pltpu.VMEM((2, nf, slots * 3 // 2, wide), BF16),
        pltpu.VMEM((2, nf, slots * 3 // 2, wide), BF16),
        pltpu.VMEM((2, nf, slots // 2, wide), BF16),
    ]
    messages = [(nf, peers, n, wide) for n in width[:4]] + [(nf // 2, peers, 24, wide)]
    scratch += [pltpu.VMEM(shape, BF16) for shape in messages * 2]
    scratch += [pltpu.VMEM((X, Y * C, n, columns), BF16) for n in width]
    scratch += [pltpu.VMEM((peers, n, columns), BF16) for n in width]
    scratch += [
        pltpu.VMEM((Z, slots, columns), BF16),
        pltpu.VMEM((Z, slots, columns), BF16),
        pltpu.VMEM((Z, 2, rows), I32),
        pltpu.VMEM((8, rows), F32),
        pltpu.VMEM((2, peers * 24, rows), BF16),
        pltpu.VMEM((2, slots * 3 // 2, rows), BF16),
        pltpu.VMEM((X, rows // X, 8), F32),
        pltpu.VMEM((X, rows // X, experts), F32),
        pltpu.VMEM((X - 1, rows // X, experts), F32),
        pltpu.VMEM((X, rows // X, 128), F32),
        pltpu.VMEM((4, Y * C * 24, hidden // 4), BF16),
        pltpu.VMEM((2, rows, columns), F32),
        pltpu.VMEM((2, 4, Y * C * 24, hidden // 4), F32),
        pltpu.VMEM((Y * C * 16, depth // 4), BF16),
    ]
    scratch += [
        dma((3,)), dma((nf,)), pltpu.SemaphoreType.REGULAR((7,)), dma((4,)), dma((2, 4, nf)), dma((5,)), dma((5, nf)),
        dma((5,)), dma((5,)), dma((1,)), dma((Z,)), dma((3,)), dma((3,)),
    ]
    return pl.pallas_call(
        kernel,
        out_shape=jax.ShapeDtypeStruct((rows, columns), BF16),
        in_specs=[any_space, any_space, vmem, vmem, any_space, any_space],
        out_specs=vmem,
        scratch_shapes=scratch,
        compiler_params=pltpu.CompilerParams(
            collective_id=0, has_side_effects=True, vmem_limit_bytes=67043328
        ),
    )(samples, gate_weight, expert_ids.T, pad_mask,
      up_weight.reshape(X, nf, wide, hidden), down_weight)


def solution(mesh):
    placed = (
        P("expert", "gate"),
        P("gate", None),
        P("expert", None),
        P("expert"),
        P(("expert", "gate"), None, None),
        P(("expert", "gate"), None, None),
    )
    return jax.shard_map(
        per_device, mesh=mesh, in_specs=placed, out_specs=P("expert", "gate"), check_vma=False
    )
```
